256 devices in a mesh: seg: 64 (over z, x, core), mp: 4 (over y).
Axes of the slice: x: 4, y: 4, z: 8, core: 2. Of those that a mesh axis runs over, the one named last changes fastest.
Arguments:
- embedded: bfloat16 [32768, 1024], P('seg'), may hold values from -6 to 6
- targets: int32 [32768], P('seg'), may hold values from 0 to 10239
- pred_device: int32 [64], P('seg'), may hold values from -1 to 63, as said below
- doc_ids: int32 [64], P('seg'), may hold values from 0 to 15, as said below
- valid_rows: int32 [64], P('seg'), may hold values from 1 to 512, as said below
- w_query: bfloat16 [1024, 1024], P(None, 'mp'), may hold values from -8 to 8
- w_key: bfloat16 [1024, 1024], P(None, 'mp'), may hold values from -1 to 1
- w_value: bfloat16 [1024, 1024], P(None, 'mp'), may hold values from -0.1875 to 0.1875
- w_rel: bfloat16 [1024, 1024], P(None, 'mp'), may hold values from -0.1875 to 0.1875
- content_bias: float32 [16, 64], P('mp'), may hold values from -3 to 3
- position_bias: float32 [16, 64], P('mp'), may hold values from -8 to 8
- attn_out: bfloat16 [1024, 1024], P('mp'), may hold values from -0.1875 to 0.1875
- attn_gain: float32 [1024], replicated, may hold values from 0.25 to 1.75
- attn_shift: float32 [1024], replicated, may hold values from -3 to 3
- w_up: bfloat16 [1024, 4096], P(None, 'mp'), may hold values from -0.1875 to 0.1875
- up_bias: float32 [4096], P('mp'), may hold values from -3 to 3
- w_down: bfloat16 [4096, 1024], P('mp'), may hold values from -0.09375 to 0.09375
- down_bias: float32 [1024], replicated, may hold values from -3 to 3
- ffn_gain: float32 [1024], replicated, may hold values from 0.25 to 1.75
- ffn_shift: float32 [1024], replicated, may hold values from -3 to 3
- w_vocab: bfloat16 [1024, 10240], P(None, 'mp'), may hold values from -8 to 8
Outputs:
- token_loglik: float32 [32768], P('seg')
- doc_loglik: float32 [16], replicated
The draws below stay inside these ranges and needn't reach their ends.
Inputs may be any that keep to these rules, and one draw needn't show every extreme that they name: `pred_device`: -1 for the first segment of a document, else the device of the document's previous segment, which lies from 3 devices below to 1 devices above; no device is named by two devices. `doc_ids`: every document holds one or more whole segments, chained by pred_device. `valid_rows`: 512 except on the last segment of a document.
All inputs are finite; a program needn't handle non-finite values.
Results may differ from the reference program's by a relative error of at most 0.007.
Values may be sent and summed in bfloat16 or wider, within the bound.
A program may use at most 128 MiB of HBM per device.

```python
import math
import jax
import jax.numpy as jnp
import numpy as np
from jax import lax

D = 1024
H = 16
DH = 64
FF = 4096
VOCAB = 10240
SEG = 512
SPREAD = 2
TOKENS = 32768
DOCS = 16
N_SEG = 64
N_MP = 4


def layout(key):
    base_key = jax.random.fold_in(key, 4301)
    cut_key = jax.random.fold_in(base_key, 1)
    order_key = jax.random.fold_in(base_key, 2)
    fill_key = jax.random.fold_in(base_key, 3)
    cut_points = jax.random.permutation(cut_key, N_SEG - 1)[:DOCS - 1] + 1
    starts = jnp.zeros((N_SEG,), jnp.int32).at[0].set(1).at[cut_points].set(1)
    doc_order = jnp.cumsum(starts) - 1
    block_keys = jax.random.split(order_key, N_SEG // SPREAD)
    shuffle = jax.vmap(lambda block_key: jax.random.permutation(block_key, SPREAD))(block_keys)
    placed = jnp.arange(N_SEG) // SPREAD * SPREAD + shuffle.reshape(-1)
    placed = placed.astype(jnp.int32)
    before = jnp.concatenate([jnp.full((1,), -1, jnp.int32), placed[:-1]])
    pred_order = jnp.where(starts == 1, -1, before)
    closing = jnp.concatenate([starts[1:], jnp.ones((1,), jnp.int32)])
    fill_rows = jax.random.randint(fill_key, (N_SEG,), 1, SEG + 1)
    valid_order = jnp.where(closing == 1, fill_rows, SEG)
    pred_device = jnp.zeros((N_SEG,), jnp.int32).at[placed].set(pred_order)
    doc_ids = jnp.zeros((N_SEG,), jnp.int32).at[placed].set(doc_order.astype(jnp.int32))
    valid_rows = jnp.zeros((N_SEG,), jnp.int32).at[placed].set(valid_order.astype(jnp.int32))
    return (pred_device, doc_ids, valid_rows)


def draw_pred_device(key, part):
    return layout(key)[0]


def draw_doc_ids(key, part):
    return layout(key)[1]


def draw_valid_rows(key, part):
    return layout(key)[2]


def projection_pair(key):
    shape_qk = (D, H * DH)
    key_base = jax.random.fold_in(key, 4101)
    query_base = jax.random.fold_in(key, 4102)
    key_part = jnp.clip(jax.random.normal(key_base, shape_qk, jnp.float32), -6.0, 6.0) * D ** (-0.5)
    query_part = jnp.clip(jax.random.normal(query_base, shape_qk, jnp.float32), -6.0, 6.0) * D ** (-0.5)
    return (query_part, key_part)


def draw_w_query(key, part):
    return projection_pair(key)[0].astype(jnp.bfloat16)


def draw_w_key(key, part):
    return projection_pair(key)[1].astype(jnp.bfloat16)


def draw_w_vocab(key, part):
    shape_out = (D, VOCAB)
    entry_key = jax.random.fold_in(key, 4201)
    return (jnp.clip(jax.random.normal(entry_key, shape_out, jnp.float32), -6.0, 6.0) * 0.1).astype(jnp.bfloat16)


def place_ends(array, rng, least, top_value):
    shape = array.shape
    spot = [jax.random.randint(jax.random.fold_in(rng, axis), (), 0, shape[axis]) for axis in range(len(shape))]
    array = array.at[tuple(spot)].set(least)
    longest = shape.index(max(shape))
    spot[longest] = (spot[longest] + 1) % shape[longest]
    return array.at[tuple(spot)].set(top_value)


def block_scale(key, dims, cuts, smallest, high):
    loudness, own = 1.0, jax.random.fold_in(key, 6)
    for axis_at, shards_of in cuts:
        heights = jnp.exp(jax.random.uniform(jax.random.fold_in(own, axis_at), (shards_of,), jnp.float32, smallest / len(cuts), high / len(cuts)))
        loudness = loudness * jnp.repeat(heights, dims[axis_at] // shards_of).reshape([-1 if axis == axis_at else 1 for axis in range(len(dims))])
    return loudness


def rank_table(amount, slope):
    loads = [(1 << 20) // math.isqrt(standing ** slope) + 1 for standing in range(1, amount + 1)]
    scale = 1 + sum(loads) // (1 << 30)
    return np.cumsum(np.array([max(1, weight // scale) for weight in loads]))


def ranked(stream_key, dims, number_of, lean):
    table = rank_table(number_of, lean)
    lot = jax.random.randint(jax.random.fold_in(stream_key, 1), dims, 0, int(table[number_of - 1]))
    standing = jnp.searchsorted(jnp.asarray(table, jnp.int32), lot, side="right")
    return jax.random.permutation(jax.random.fold_in(stream_key, 2), number_of)[standing].astype(jnp.int32)


def noise(key, extent, scale, bound, cuts=(), dtype=jnp.bfloat16):
    loudness = block_scale(key, extent, cuts, -0.22, 0.18) if cuts else 1.0
    result = jax.random.normal(key, extent, jnp.float32) * scale * loudness
    return jnp.minimum(jnp.maximum(result, -bound), bound).astype(dtype)


def setup_inputs(seed: int = 0) -> dict:
    streams_of = jax.random.split(jax.random.key(seed), 22)
    return {
        "embedded": noise(streams_of[0], (TOKENS, D), 1.0, 6.0, ((0, 64),)),
        "targets": place_ends(ranked(streams_of[1], (TOKENS,), VOCAB, 2), jax.random.fold_in(streams_of[1], 3), 0, VOCAB - 1).astype(jnp.int32),
        "pred_device": draw_pred_device(jax.random.fold_in(streams_of[21], 71), 0),
        "doc_ids": draw_doc_ids(jax.random.fold_in(streams_of[21], 71), 0),
        "valid_rows": draw_valid_rows(jax.random.fold_in(streams_of[21], 71), 0),
        "w_query": draw_w_query(jax.random.fold_in(streams_of[21], 71), 0),
        "w_key": draw_w_key(jax.random.fold_in(streams_of[21], 71), 0),
        "w_value": noise(streams_of[7], (D, H * DH), D ** -0.5, 0.1875, ((1, 4),)),
        "w_rel": noise(streams_of[8], (D, H * DH), D ** -0.5, 0.1875, ((1, 4),)),
        "content_bias": noise(streams_of[9], (H, DH), 0.5, 3.0, ((0, 4),), jnp.float32),
        "position_bias": noise(streams_of[10], (H, DH), 2.0, 8.0, ((0, 4),), jnp.float32),
        "attn_out": noise(streams_of[11], (H * DH, D), (H * DH) ** -0.5, 0.1875, ((0, 4),)),
        "attn_gain": jnp.clip(1.0 + 0.15 * jax.random.normal(streams_of[12], (D,), jnp.float32), 0.25, 1.75),
        "attn_shift": noise(streams_of[13], (D,), 0.5, 3.0, (), jnp.float32),
        "w_up": noise(streams_of[14], (D, FF), D ** -0.5, 0.1875, ((1, 4),)),
        "up_bias": noise(streams_of[15], (FF,), 0.5, 3.0, ((0, 4),), jnp.float32),
        "w_down": noise(streams_of[16], (FF, D), FF ** -0.5, 0.09375, ((0, 4),)),
        "down_bias": noise(streams_of[17], (D,), 0.5, 3.0, (), jnp.float32),
        "ffn_gain": jnp.clip(1.0 + 0.15 * jax.random.normal(streams_of[18], (D,), jnp.float32), 0.25, 1.75),
        "ffn_shift": noise(streams_of[19], (D,), 0.5, 3.0, (), jnp.float32),
        "w_vocab": draw_w_vocab(jax.random.fold_in(streams_of[21], 71), 0),
    }


EPSILON = 1e-05

def rounded(values):
    return lax.optimization_barrier(values.astype(jnp.bfloat16)).astype(jnp.float32)

def normalize(values, norm_gain, norm_shift):
    centre = values - lax.optimization_barrier(jnp.mean(values, axis=-1, keepdims=True))
    spread = lax.optimization_barrier(jnp.mean(centre * centre, axis=-1, keepdims=True))
    return centre * lax.rsqrt(spread + EPSILON) * norm_gain + norm_shift

def position_table(length, features):
    places = jnp.arange(length).astype(jnp.float32)
    frequency = 10000.0 ** (-jnp.arange(0, features, 2).astype(jnp.float32) / features)
    angles = places[:, None] * frequency[None, :]
    return jnp.concatenate([jnp.sin(angles), jnp.cos(angles)], axis=1).astype(jnp.bfloat16)

def group_sum(operand, matrix):
    rows_n = operand.shape[0]
    pieces = operand.reshape(rows_n, N_MP, -1).astype(jnp.float32)
    blocks = matrix.reshape(N_MP, -1, matrix.shape[1]).astype(jnp.float32)
    partial_terms = jnp.einsum('rgk,gkd->grd', pieces, blocks)
    return lax.optimization_barrier(jnp.sum(rounded(partial_terms), axis=0))

def reference(embedded, targets, pred_device, doc_ids, valid_rows, w_query, w_key, w_value, w_rel, content_bias, position_bias, attn_out, attn_gain, attn_shift, w_up, up_bias, w_down, down_bias, ffn_gain, ffn_shift, w_vocab):
    head_count = content_bias.shape[0]
    head_dim = content_bias.shape[1]
    key_span = 2 * SEG
    score_scale = head_dim ** (-0.5)
    rel_keys = jnp.dot(position_table(key_span, D), w_rel, preferred_element_type=jnp.float32)
    rel_keys = rounded(rel_keys).reshape(key_span, head_count, head_dim)
    segments = embedded.reshape(N_SEG, SEG, D)
    memories = segments[jnp.maximum(pred_device, 0)]
    row_index = jnp.arange(SEG)[:, None]
    key_index = jnp.arange(key_span)[None, :]
    distance = row_index + SEG - key_index
    gather_index = jnp.clip(distance, 0, key_span - 1).astype(jnp.int32)
    causal = distance >= 0

    def one_segment(segment_items):
        current, memory, has_memory, target_rows, used_rows = segment_items
        keys_in = jnp.concatenate([memory, current], axis=0)
        queries = jnp.dot(current, w_query, preferred_element_type=jnp.float32)
        with_content = rounded(queries + content_bias.reshape(-1)).reshape(SEG, head_count, head_dim)
        with_position = rounded(queries + position_bias.reshape(-1)).reshape(SEG, head_count, head_dim)
        key_rows = rounded(jnp.dot(keys_in, w_key, preferred_element_type=jnp.float32)).reshape(key_span, head_count, head_dim)
        value_rows = rounded(jnp.dot(keys_in, w_value, preferred_element_type=jnp.float32)).reshape(key_span, head_count, head_dim)
        content_score = jnp.einsum('ihd,jhd->hij', with_content, key_rows)
        position_all = jnp.einsum('ihd,rhd->hir', with_position, rel_keys)
        position_score = jnp.take_along_axis(position_all, jnp.broadcast_to(gather_index[None], position_all.shape), axis=2)
        allowed = causal & ((key_index >= SEG) | has_memory)
        scores = jnp.where(allowed[None], (content_score + position_score) * score_scale, -1e+30)
        row_top = lax.optimization_barrier(jnp.max(scores, axis=-1, keepdims=True))
        exponent = jnp.where(allowed[None], jnp.exp(scores - row_top), 0.0)
        row_total = lax.optimization_barrier(jnp.sum(exponent, axis=-1, keepdims=True))
        weights = rounded(exponent / row_total)
        attended = jnp.einsum('hij,jhd->ihd', weights, value_rows).astype(jnp.bfloat16).reshape(SEG, head_count * head_dim)
        attended_sum = group_sum(attended, attn_out)
        first_out = normalize(current.astype(jnp.float32) + attended_sum, attn_gain, attn_shift).astype(jnp.bfloat16)
        units = jnp.maximum(jnp.dot(first_out, w_up, preferred_element_type=jnp.float32) + up_bias, 0.0).astype(jnp.bfloat16)
        ffn_out = group_sum(units, w_down)
        second = normalize(first_out.astype(jnp.float32) + ffn_out + down_bias, ffn_gain, ffn_shift).astype(jnp.bfloat16)
        logits = jnp.dot(second, w_vocab, preferred_element_type=jnp.float32)
        logit_top = lax.optimization_barrier(jnp.max(logits, axis=1))
        log_total = logit_top + jnp.log(lax.optimization_barrier(jnp.sum(jnp.exp(logits - logit_top[:, None]), axis=1)))
        picked = jnp.take_along_axis(logits, target_rows[:, None].astype(jnp.int32), axis=1)[:, 0]
        return jnp.where(jnp.arange(SEG) < used_rows, picked - log_total, 0.0)
    token_loglik = lax.map(one_segment, (segments, memories, pred_device >= 0, targets.reshape(N_SEG, SEG), valid_rows))
    doc_total = jax.ops.segment_sum(lax.optimization_barrier(jnp.sum(token_loglik, axis=1)), doc_ids, num_segments=DOCS)
    doc_rows = jax.ops.segment_sum(valid_rows.astype(jnp.float32), doc_ids, num_segments=DOCS)
    return (token_loglik.reshape(-1), doc_total / doc_rows)
```

```python
import functools

import jax
import jax.numpy as jnp
import numpy as np
from jax import lax
from jax.experimental import pallas as pl
from jax.experimental.pallas import tpu as pltpu
from jax.sharding import PartitionSpec as P

EPSILON = 1e-05
MESH = pl.DeviceIdType.MESH
F32, BF16 = jnp.float32, jnp.bfloat16
N_X = 4
N_MP = 4
HEADS = 4
ROWS = 512
WIDTH = 1024
BLOCK = 128
HALF = 256
PIECE = 64
FINE = 32
MASKED = -1e30


def normalize(values, gain, shift):
    centre = values - jnp.mean(values, axis=-1, keepdims=True)
    spread = jnp.mean(centre * centre, axis=-1, keepdims=True)
    return centre * lax.rsqrt(spread + EPSILON) * gain + shift


def dot(a, b):
    return jnp.dot(a, b, preferred_element_type=F32)


def dot_t(a, b):
    return lax.dot_general(a, b, (((1,), (1,)), ((), ())), preferred_element_type=F32)


def kernel(
    n_seg,
    pred_s,
    doc_s,
    valid_s,
    content_bias,
    position_bias,
    basis,
    targets,
    attn_gain,
    attn_shift,
    up_bias,
    down_bias,
    ffn_gain,
    ffn_shift,
    embedded_h,
    wq_h,
    wk_h,
    wv_h,
    wr_h,
    attn_out_h,
    wup_h,
    wdown_h,
    wvocab_h,
    token_o,
    doc_o,
    emb,
    wq,
    wk,
    wv,
    wr,
    attn_out,
    wup,
    wdown,
    wvocab,
    table,
    rel,
    qc,
    qp,
    kv_own,
    kv_same,
    kv_partner,
    kv_cross,
    kv_x,
    kv_past,
    pos_past,
    top_own,
    sum_own,
    out_own,
    att_acc,
    attended,
    first_out,
    units,
    rs_send,
    rs_recv,
    second,
    stats_col,
    stats,
    doc_a,
    doc_b,
    load_sem,
    same_s,
    same_r,
    partner_s,
    partner_r,
    cross_s,
    cross_r,
    x_s,
    x_r,
    ao_s,
    ao_r,
    aof_s,
    aof_r,
    att_s,
    att_r,
    rs_s,
    rs_r,
    ag_s,
    ag_r,
    st_s,
    st_r,
    da_s,
    da_r,
    db_s,
    db_r,
):
    seg = lax.axis_index("seg")
    mp = lax.axis_index("mp")
    core = lax.rem(seg, 2)
    chip = lax.div(seg, 2)
    n_chip = n_seg // 2
    group = 2 * N_X
    n_z = n_seg // group
    in_group = lax.rem(seg, group)
    z = lax.div(seg, group)

    def chip_at(step, c):
        return (lax.rem(chip + step + n_chip, n_chip) * 2 + c, mp)

    partner = (chip * 2 + 1 - core, mp)
    forward = chip_at(1, core)
    backward = chip_at(-1, core)

    def mp_at(k):
        return (seg, lax.rem(mp + k, N_MP))

    def group_at(k):
        return (z * group + lax.rem(in_group + k, group), mp)

    def z_at(k):
        return (lax.rem(z + k, n_z) * group + in_group, mp)

    x_to = (lax.rem(chip + n_chip + 2 * core - 1, n_chip) * 2 + 1 - core, mp)

    pending = []

    def remote(src, dst, s_sem, r_sem, device):
        return pltpu.make_async_remote_copy(
            src_ref=src,
            dst_ref=dst,
            send_sem=s_sem,
            recv_sem=r_sem,
            device_id=device,
            device_id_type=MESH,
        )

    def send(*args):
        copy = remote(*args)
        copy.start()
        pending.append(copy)

    loads = []
    own_rows = attn_out.at[mp]
    for n, (src, dst) in enumerate(
        (
            (embedded_h, emb),
            (wk_h, wk),
            (wv_h, wv),
            (attn_out_h, own_rows),
            (wq_h, wq),
            (wr_h, wr),
            (wup_h, wup),
            (wdown_h, wdown),
            (wvocab_h, wvocab),
        )
    ):
        copy = pltpu.make_async_copy(src, dst, load_sem.at[n])
        copy.start()
        loads.append(copy)

    barrier = pltpu.get_barrier_semaphore()
    friends = [partner, forward, backward, x_to]
    friends += [mp_at(k) for k in range(1, N_MP)]
    friends += [group_at(k) for k in range(1, group)]
    friends += [z_at(k) for k in range(1, n_z)]
    for friend in friends:
        pl.semaphore_signal(barrier, inc=1, device_id=friend, device_id_type=MESH)

    def kv_sends(t):
        send(kv_own.at[t], kv_same.at[t], same_s.at[t], same_r.at[t], forward)
        send(kv_own.at[t], kv_partner.at[t], partner_s.at[t], partner_r.at[t], partner)

        @pl.when(core == 0)
        def _():
            remote(kv_own.at[t], kv_x.at[t], x_s.at[t], x_r.at[t], x_to).start()

    loads[0].wait()
    loads[1].wait()
    for t in range(2):
        kv_own[t] = dot(emb[t * HALF : (t + 1) * HALF, :], wk[...]).astype(BF16)
    pl.semaphore_wait(barrier, len(friends))
    for t in range(2):
        kv_sends(t)
    loads[2].wait()
    for t in range(2):
        kv_own[2 + t] = dot(emb[t * HALF : (t + 1) * HALF, :], wv[...]).astype(BF16)
    for t in range(2, 4):
        kv_sends(t)

    loads[3].wait()
    part = pl.ds(pl.multiple_of(core * BLOCK, BLOCK), BLOCK)
    for k in range(1, N_MP):
        here = attn_out.at[mp, part]
        send(here, here, ao_s.at[k - 1], ao_r.at[k - 1], mp_at(k))

    loads[4].wait()
    for t in range(2):
        rows = slice(t * HALF, (t + 1) * HALF)
        q = dot(emb[rows, :], wq[...])
        for h in range(HEADS):
            cols = slice(h * 64, (h + 1) * 64)
            qc[rows, cols] = (q[:, cols] + content_bias[h : h + 1, :]).astype(BF16)
            qp[rows, cols] = (q[:, cols] + position_bias[h : h + 1, :]).astype(BF16)

    loads[5].wait()
    rel[WIDTH:, :] = jnp.zeros((BLOCK, HALF), BF16)

    def rel_block(n, carry):
        for k in range(HALF // FINE):
            at = n * (HALF // FINE) + k
            sin_a, cos_a = basis[0, pl.ds(at, 1), :], basis[1, pl.ds(at, 1), :]
            sin_b, cos_b = basis[2], basis[3]
            rows = slice(k * FINE, (k + 1) * FINE)
            table[rows, : WIDTH // 2] = (sin_a * cos_b + cos_a * sin_b).astype(BF16)
            table[rows, WIDTH // 2 :] = (cos_a * cos_b - sin_a * sin_b).astype(BF16)
        rel[pl.ds(pl.multiple_of(n * HALF, HALF), HALF), :] = dot(table[...], wr[...]).astype(BF16)
        return carry

    lax.fori_loop(0, WIDTH // HALF, rel_block, 0)

    lanes = lax.broadcasted_iota(jnp.int32, (BLOCK, HALF), 1)
    row_at = lax.broadcasted_iota(jnp.int32, (BLOCK, BLOCK), 0)
    col_at = lax.broadcasted_iota(jnp.int32, (BLOCK, BLOCK), 1)

    def of_head(h):
        return (lanes >= h * 64) & (lanes < h * 64 + 64)

    def one_head(ref, rows, mine):
        values = ref[rows, :].astype(F32) * 0.125
        return jnp.where(mine, values, 0.0).astype(BF16)

    def relay(t):
        remote(kv_own.at[t], kv_same.at[t], same_s.at[t], same_r.at[t], forward).wait_recv()
        send(kv_same.at[t], kv_cross.at[t], cross_s.at[t], cross_r.at[t], partner)

        @pl.when(core == 1)
        def _():
            remote(kv_same.at[t], kv_x.at[t], x_s.at[t], x_r.at[t], x_to).start()

    for b in range(ROWS // BLOCK):
        rows = slice(b * BLOCK, (b + 1) * BLOCK)
        own = (b + 1) * BLOCK
        begin = ROWS - own
        width = WIDTH + BLOCK - begin

        def own_part(h, carry, rows=rows, own=own, begin=begin, width=width):
            mine = of_head(h)
            near = dot_t(one_head(qp, rows, mine), rel[begin:, :])
            near = pltpu.roll(near, width - BLOCK + 1, 1, stride=1, stride_axis=0)
            pos_past[h, rows, :] = near[:, :ROWS]
            keys = []
            for c in range(2):
                if own > c * HALF:
                    keys.append(kv_own[c, : min(HALF, own - c * HALF), :])
            query = one_head(qc, rows, mine)
            content = [dot_t(query, piece) for piece in keys]
            content = content[0] if len(content) == 1 else jnp.concatenate(content, axis=1)
            score = content + near[:, ROWS : ROWS + own]
            last = jnp.where(col_at <= row_at, score[:, own - BLOCK :], MASKED)
            score = last if own == BLOCK else jnp.concatenate([score[:, : own - BLOCK], last], axis=1)
            top = jnp.max(score, axis=-1, keepdims=True)
            weight = jnp.exp(score - top)
            top_own[h, rows, :] = top
            sum_own[h, rows, :] = jnp.sum(weight, axis=-1, keepdims=True)
            weight = weight.astype(BF16)
            total = None
            for c, piece in enumerate(keys):
                n = piece.shape[0]
                term = dot(weight[:, c * HALF : c * HALF + n], kv_own[2 + c, :n, :])
                total = term if total is None else total + term
            out_own[rows, :] = jnp.where(mine, total, out_own[rows, :])
            return carry

        out_own[rows, :] = jnp.zeros((BLOCK, HALF), F32)
        lax.fori_loop(0, HEADS, own_part, 0)
        relay(b)

    for k in range(1, N_MP):
        there = lax.rem(mp + N_MP - k, N_MP)
        here = attn_out.at[there, part]
        remote(here, here, ao_s.at[k - 1], ao_r.at[k - 1], mp_at(k)).wait_recv()
        send(here, here, aof_s.at[k - 1], aof_r.at[k - 1], partner)

    behind = seg - pred_s[0]
    has_memory = pred_s[0] >= 0
    use_cross = behind == 1 + 2 * core
    use_partner = behind == 2 * core - 1
    use_x = behind == 3 - 4 * core
    for t in range(4):
        remote(kv_own.at[t], kv_partner.at[t], partner_s.at[t], partner_r.at[t], partner).wait_recv()
        remote(kv_same.at[t], kv_cross.at[t], cross_s.at[t], cross_r.at[t], partner).wait_recv()
        remote(kv_same.at[t], kv_x.at[t], x_s.at[t], x_r.at[t], x_to).wait_recv()
        chosen = jnp.where(use_cross, kv_cross[t], kv_same[t])
        chosen = jnp.where(use_partner, kv_partner[t], chosen)
        kv_past[t] = jnp.where(use_x, kv_x[t], chosen)

    for b in range(ROWS // BLOCK):
        rows = slice(b * BLOCK, (b + 1) * BLOCK)

        def past_part(h, carry, rows=rows):
            mine = of_head(h)
            query = one_head(qc, rows, mine)
            score = jnp.concatenate([dot_t(query, kv_past[c]) for c in range(2)], axis=1)
            score = jnp.where(has_memory, score + pos_past[h, rows, :], MASKED)
            before = top_own[h, rows, :]
            top = jnp.maximum(before, jnp.max(score, axis=-1, keepdims=True))
            weight = jnp.exp(score - top)
            fade = jnp.exp(before - top)
            total = sum_own[h, rows, :] * fade + jnp.sum(weight, axis=-1, keepdims=True)
            weight = weight.astype(BF16)
            past = dot(weight[:, :HALF], kv_past[2]) + dot(weight[:, HALF:], kv_past[3])
            done = (out_own[rows, :] * fade + past) / total
            att_acc[...] = jnp.where(mine, done, att_acc[...])
            return carry

        att_acc[...] = jnp.zeros((BLOCK, HALF), F32)
        lax.fori_loop(0, HEADS, past_part, 0)
        attended[mp, rows, :] = att_acc[...].astype(BF16)
        for k in range(1, N_MP):
            here = attended.at[mp, rows]
            send(here, here, att_s.at[k - 1, b], att_r.at[k - 1, b], mp_at(k))

    for k in range(1, N_MP):
        there = lax.rem(mp + N_MP - k, N_MP)
        other = pl.ds(pl.multiple_of((1 - core) * BLOCK, BLOCK), BLOCK)
        here = attn_out.at[there, other]
        remote(here, here, aof_s.at[k - 1], aof_r.at[k - 1], partner).wait_recv()
    loads[6].wait()
    loads[7].wait()
    loads[8].wait()

    for half in range(2):
        rows = slice(half * HALF, (half + 1) * HALF)
        for b in range(2 * half, 2 * half + 2):
            for k in range(1, N_MP):
                there = lax.rem(mp + N_MP - k, N_MP)
                here = attended.at[there, b * BLOCK : (b + 1) * BLOCK]
                remote(here, here, att_s.at[k - 1, b], att_r.at[k - 1, b], mp_at(k)).wait_recv()
        total = emb[rows, :].astype(F32)
        head_sum = None
        for g in range(N_MP):
            term = dot(attended[g, rows, :], attn_out[g]).astype(BF16).astype(F32)
            head_sum = term if head_sum is None else head_sum + term
        first = normalize(total + head_sum, attn_gain[...], attn_shift[...]).astype(BF16)
        first_out[rows, :] = first
        units[...] = jnp.maximum(dot(first, wup[...]) + up_bias[...], 0.0).astype(BF16)
        terms = dot(units[...], wdown[...]).astype(BF16)
        for d in range(N_MP):
            rs_send[half, d] = terms[d * PIECE : (d + 1) * PIECE, :]
        for k in range(1, N_MP):
            to = lax.rem(mp + k, N_MP)
            send(rs_send.at[half, to], rs_recv.at[half, k - 1], rs_s.at[k - 1, half], rs_r.at[k - 1, half], mp_at(k))

    for half in range(2):
        total = rs_send[half, mp].astype(F32)
        for k in range(1, N_MP):
            to = lax.rem(mp + k, N_MP)
            remote(rs_send.at[half, to], rs_recv.at[half, k - 1], rs_s.at[k - 1, half], rs_r.at[k - 1, half], mp_at(k)).wait_recv()
            total = total + rs_recv[half, k - 1].astype(F32)
        at = pl.ds(pl.multiple_of(half * HALF + mp * PIECE, PIECE), PIECE)
        total = first_out[at, :].astype(F32) + total + down_bias[...]
        second[half, mp] = normalize(total, ffn_gain[...], ffn_shift[...]).astype(BF16)
        for k in range(1, N_MP):
            here = second.at[half, mp]
            send(here, here, ag_s.at[k - 1, half], ag_r.at[k - 1, half], mp_at(k))

    tile = 512
    n_words = wvocab_h.shape[1]
    for half in range(2):
        rows = slice(half * HALF, (half + 1) * HALF)
        for k in range(1, N_MP):
            there = lax.rem(mp + N_MP - k, N_MP)
            here = second.at[half, there]
            remote(here, here, ag_s.at[k - 1, half], ag_r.at[k - 1, half], mp_at(k)).wait_recv()
        states = jnp.concatenate([second[half, d] for d in range(N_MP)], axis=0)
        wanted = targets[rows, :] - mp * n_words
        words = lax.broadcasted_iota(jnp.int32, (HALF, tile), 1)

        def vocab_tile(n, carry, states=states, wanted=wanted, words=words):
            top, total, picked = carry
            at = pl.multiple_of(n * tile, tile)
            logits = dot(states, wvocab[:, pl.ds(at, tile)])
            new_top = jnp.maximum(top, jnp.max(logits, axis=1, keepdims=True))
            total = total * jnp.exp(top - new_top)
            total = total + jnp.sum(jnp.exp(logits - new_top), axis=1, keepdims=True)
            hit = jnp.where(words == wanted - at, logits, 0.0)
            return new_top, total, picked + jnp.sum(hit, axis=1, keepdims=True)

        zero = jnp.zeros((HALF, 1), F32)
        top, total, picked = lax.fori_loop(
            0, n_words // tile, vocab_tile, (jnp.full((HALF, 1), -jnp.inf, F32), zero, zero)
        )
        lane = lax.broadcasted_iota(jnp.int32, (HALF, BLOCK), 1)
        packed = jnp.where(lane == 0, top, jnp.where(lane == 1, total, picked))
        stats[mp, :, rows] = jnp.transpose(packed)[:8, :]

    for k in range(1, N_MP):
        here = stats.at[mp]
        send(here, here, st_s.at[k - 1], st_r.at[k - 1], mp_at(k))
    for k in range(1, N_MP):
        there = lax.rem(mp + N_MP - k, N_MP)
        here = stats.at[there]
        remote(here, here, st_s.at[k - 1], st_r.at[k - 1], mp_at(k)).wait_recv()
    top = stats[0, 0:1, :]
    for g in range(1, N_MP):
        top = jnp.maximum(top, stats[g, 0:1, :])
    total, picked = None, None
    for g in range(N_MP):
        term = stats[g, 1:2, :] * jnp.exp(stats[g, 0:1, :] - top)
        total = term if total is None else total + term
        picked = stats[g, 2:3, :] if picked is None else picked + stats[g, 2:3, :]
    position = lax.broadcasted_iota(jnp.int32, (1, ROWS), 1)
    tokens = jnp.where(position < valid_s[0], picked - (top + jnp.log(total)), 0.0)
    token_o[...] = tokens

    slot = lax.broadcasted_iota(jnp.int32, (8, BLOCK), 1) == doc_s[0]
    line = lax.broadcasted_iota(jnp.int32, (8, BLOCK), 0)
    used = valid_s[0].astype(F32)
    share = jnp.sum(tokens, axis=1, keepdims=True)
    doc_a[0] = jnp.where(slot, jnp.where(line == 0, share, jnp.where(line == 1, used, 0.0)), 0.0)
    for k in range(1, group):
        send(doc_a.at[0], doc_a.at[k], da_s.at[k - 1], da_r.at[k - 1], group_at(k))
    for k in range(1, group):
        remote(doc_a.at[0], doc_a.at[k], da_s.at[k - 1], da_r.at[k - 1], group_at(k)).wait_recv()
    doc_b[0] = jnp.sum(doc_a[...], axis=0)
    for k in range(1, n_z):
        send(doc_b.at[0], doc_b.at[k], db_s.at[k - 1], db_r.at[k - 1], z_at(k))
    for k in range(1, n_z):
        remote(doc_b.at[0], doc_b.at[k], db_s.at[k - 1], db_r.at[k - 1], z_at(k)).wait_recv()
    docs = jnp.sum(doc_b[...], axis=0)
    doc_o[...] = docs[0:1, :] / docs[1:2, :]

    for copy in pending:
        copy.wait_send()
    for t in range(4):
        remote(kv_own.at[t], kv_x.at[t], x_s.at[t], x_r.at[t], x_to).wait_send()


def angle_basis():
    frequency = 10000.0 ** (-np.arange(0, WIDTH, 2, dtype=np.float64) / WIDTH)
    coarse = (WIDTH // FINE - 1 - np.arange(WIDTH // FINE))[:, None] * FINE * frequency[None, :]
    fine = (FINE - 1 - np.arange(FINE))[:, None] * frequency[None, :]
    return np.stack([np.sin(coarse), np.cos(coarse), np.sin(fine), np.cos(fine)]).astype(np.float32)


def on_device(
    n_seg,
    embedded,
    targets,
    pred_device,
    doc_ids,
    valid_rows,
    w_query,
    w_key,
    w_value,
    w_rel,
    content_bias,
    position_bias,
    attn_out,
    attn_gain,
    attn_shift,
    w_up,
    up_bias,
    w_down,
    down_bias,
    ffn_gain,
    ffn_shift,
    w_vocab,
):
    smem = pl.BlockSpec(memory_space=pltpu.SMEM)
    vmem = pl.BlockSpec(memory_space=pltpu.VMEM)
    hbm = pl.BlockSpec(memory_space=pl.ANY)
    dma = pltpu.SemaphoreType.DMA
    words = w_vocab.shape[1]
    n_z = n_seg // (2 * N_X)
    kv = pltpu.VMEM((4, HALF, HALF), BF16)
    weight = pltpu.VMEM((WIDTH, HALF), BF16)
    column = pltpu.VMEM((HEADS, ROWS, 1), F32)
    scratch = [
        pltpu.VMEM((ROWS, WIDTH), BF16),
        weight,
        weight,
        weight,
        weight,
        pltpu.VMEM((N_MP, HALF, WIDTH), BF16),
        pltpu.VMEM((WIDTH, WIDTH), BF16),
        pltpu.VMEM((WIDTH, WIDTH), BF16),
        pltpu.VMEM((WIDTH, words), BF16),
        pltpu.VMEM((HALF, WIDTH), BF16),
        pltpu.VMEM((WIDTH + BLOCK, HALF), BF16),
        pltpu.VMEM((ROWS, HALF), BF16),
        pltpu.VMEM((ROWS, HALF), BF16),
        kv,
        kv,
        kv,
        kv,
        kv,
        kv,
        pltpu.VMEM((HEADS, ROWS, ROWS), F32),
        column,
        column,
        pltpu.VMEM((ROWS, HALF), F32),
        pltpu.VMEM((BLOCK, HALF), F32),
        pltpu.VMEM((N_MP, ROWS, HALF), BF16),
        pltpu.VMEM((ROWS, WIDTH), BF16),
        pltpu.VMEM((HALF, WIDTH), BF16),
        pltpu.VMEM((2, N_MP, PIECE, WIDTH), BF16),
        pltpu.VMEM((2, N_MP - 1, PIECE, WIDTH), BF16),
        pltpu.VMEM((2, N_MP, PIECE, WIDTH), BF16),
        pltpu.VMEM((8, BLOCK), F32),
        pltpu.VMEM((N_MP, 8, ROWS), F32),
        pltpu.VMEM((2 * N_X, 8, BLOCK), F32),
        pltpu.VMEM((n_z, 8, BLOCK), F32),
        dma((9,)),
    ]
    scratch += [dma((4,))] * 8
    scratch += [dma((N_MP - 1,))] * 4
    scratch += [dma((N_MP - 1, 4))] * 2
    scratch += [dma((N_MP - 1, 2))] * 4
    scratch += [dma((N_MP - 1,))] * 2
    scratch += [dma((2 * N_X - 1,))] * 2
    scratch += [dma((n_z - 1,))] * 2
    token_terms, docs = pl.pallas_call(
        functools.partial(kernel, n_seg),
        out_shape=(
            jax.ShapeDtypeStruct((1, ROWS), F32),
            jax.ShapeDtypeStruct((1, BLOCK), F32),
        ),
        in_specs=[smem] * 3 + [vmem] * 10 + [hbm] * 9,
        out_specs=(vmem, vmem),
        scratch_shapes=scratch,
        compiler_params=pltpu.CompilerParams(
            collective_id=0, has_side_effects=True, vmem_limit_bytes=60 * 1024 * 1024
        ),
        name="layer",
    )(
        pred_device,
        doc_ids,
        valid_rows,
        content_bias,
        position_bias,
        jnp.asarray(angle_basis()),
        targets.reshape(ROWS, 1),
        attn_gain.reshape(1, WIDTH),
        attn_shift.reshape(1, WIDTH),
        up_bias.reshape(1, WIDTH),
        down_bias.reshape(1, WIDTH),
        ffn_gain.reshape(1, WIDTH),
        ffn_shift.reshape(1, WIDTH),
        embedded,
        w_query,
        w_key,
        w_value,
        w_rel,
        attn_out,
        w_up,
        w_down,
        w_vocab,
    )
    doc_slots = n_seg // 4
    return token_terms.reshape(ROWS), docs[0, :doc_slots]


def solution(mesh):
    return jax.shard_map(
        functools.partial(on_device, mesh.shape["seg"]),
        mesh=mesh,
        in_specs=(
            P("seg", None),
            P("seg"),
            P("seg"),
            P("seg"),
            P("seg"),
            P(None, "mp"),
            P(None, "mp"),
            P(None, "mp"),
            P(None, "mp"),
            P("mp", None),
            P("mp", None),
            P("mp", None),
            P(),
            P(),
            P(None, "mp"),
            P("mp"),
            P("mp", None),
            P(),
            P(),
            P(),
            P(None, "mp"),
        ),
        out_specs=(P("seg"), P()),
        check_vma=False,
    )
```

```python
import functools

import jax
import jax.numpy as jnp
import numpy as np
from jax import lax
from jax.experimental import pallas as pl
from jax.experimental.pallas import tpu as pltpu
from jax.sharding import PartitionSpec as P

EPSILON = 1e-05
MESH = pl.DeviceIdType.MESH
F32, BF16 = jnp.float32, jnp.bfloat16
N_X = 4
N_MP = 4
HEADS = 4
ROWS = 512
WIDTH = 1024
BLOCK = 128
HALF = 256
PIECE = 64
FINE = 32
MASKED = -1e30


def normalize(values, gain, shift):
    centre = values - jnp.mean(values, axis=-1, keepdims=True)
    spread = jnp.mean(centre * centre, axis=-1, keepdims=True)
    return centre * lax.rsqrt(spread + EPSILON) * gain + shift


def dot(a, b):
    return jnp.dot(a, b, preferred_element_type=F32)


def dot_t(a, b):
    return lax.dot_general(a, b, (((1,), (1,)), ((), ())), preferred_element_type=F32)


def kernel(
    n_seg,
    pred_v,
    doc_v,
    valid_v,
    content_bias_h,
    position_bias_h,
    basis_h,
    targets_h,
    attn_gain_h,
    attn_shift_h,
    up_bias_h,
    down_bias_h,
    ffn_gain_h,
    ffn_shift_h,
    embedded_h,
    wq_h,
    wk_h,
    wv_h,
    wr_h,
    attn_out_h,
    wup_h,
    wdown_h,
    wvocab_h,
    token_o,
    doc_o,
    content_bias,
    position_bias,
    basis,
    targets,
    attn_gain,
    attn_shift,
    up_bias,
    down_bias,
    ffn_gain,
    ffn_shift,
    emb,
    wq,
    wk,
    wv,
    wr,
    attn_out,
    wup,
    wdown,
    wvocab,
    table,
    rel,
    qc,
    qp,
    kv_own,
    kv_same,
    kv_partner,
    kv_cross,
    kv_x,
    kv_past,
    pos_past,
    top_own,
    sum_own,
    out_own,
    attended,
    first_out,
    units,
    rs_send,
    rs_recv,
    rs_pass,
    second,
    target_col,
    stats,
    doc_a,
    doc_b,
    load_sem,
    same_s,
    same_r,
    partner_s,
    partner_r,
    cross_s,
    cross_r,
    x_s,
    x_r,
    ao_s,
    ao_r,
    aof_s,
    aof_r,
    att_s,
    att_r,
    rs_s,
    rs_r,
    ag_s,
    ag_r,
    st_s,
    st_r,
    da_s,
    da_r,
    db_s,
    db_r,
):
    seg = lax.axis_index("seg")
    mp = lax.axis_index("mp")
    core = lax.rem(seg, 2)
    chip = lax.div(seg, 2)
    n_chip = n_seg // 2
    group = 2 * N_X
    n_z = n_seg // group
    in_group = lax.rem(seg, group)
    z = lax.div(seg, group)

    def chip_at(step, c):
        return (lax.rem(chip + step + n_chip, n_chip) * 2 + c, mp)

    partner = (chip * 2 + 1 - core, mp)
    forward = chip_at(1, core)
    backward = chip_at(-1, core)

    def mp_at(k):
        return (seg, lax.rem(mp + k, N_MP))

    def group_at(k):
        return (z * group + lax.rem(in_group + k, group), mp)

    def z_at(k):
        return (lax.rem(z + k, n_z) * group + in_group, mp)

    x_to = (lax.rem(chip + n_chip + 2 * core - 1, n_chip) * 2 + 1 - core, mp)

    pending = []

    def remote(src, dst, s_sem, r_sem, device):
        return pltpu.make_async_remote_copy(
            src_ref=src,
            dst_ref=dst,
            send_sem=s_sem,
            recv_sem=r_sem,
            device_id=device,
            device_id_type=MESH,
        )

    def send(*args):
        copy = remote(*args)
        copy.start()
        pending.append(copy)

    sources = (
        (embedded_h, emb),
        (wk_h, wk),
        (wv_h, wv),
        (attn_out_h, attn_out.at[mp]),
        (wq_h, wq),
        (wr_h, wr),
        (wup_h, wup),
        (wdown_h, wdown),
        (wvocab_h, wvocab),
        (content_bias_h, content_bias),
        (position_bias_h, position_bias),
        (basis_h, basis),
        (targets_h, targets),
        (attn_gain_h, attn_gain),
        (attn_shift_h, attn_shift),
        (up_bias_h, up_bias),
        (down_bias_h, down_bias),
        (ffn_gain_h, ffn_gain),
        (ffn_shift_h, ffn_shift),
    )
    loads = [pltpu.make_async_copy(src, dst, load_sem.at[n]) for n, (src, dst) in enumerate(sources)]
    for n in (0, 1, 2, 4, 9, 10, 11, 5, 3, *range(12, 19)):
        loads[n].start()

    barrier = pltpu.get_barrier_semaphore()
    friends = [partner, forward, backward, x_to]
    friends += [mp_at(k) for k in range(1, N_MP)]
    friends += [group_at(k) for k in range(1, group)]
    friends += [z_at(k) for k in range(1, n_z)]
    for friend in friends:
        pl.semaphore_signal(barrier, inc=1, device_id=friend, device_id_type=MESH)

    def kv_sends(t):
        send(kv_own.at[t], kv_same.at[t], same_s.at[t], same_r.at[t], forward)
        send(kv_own.at[t], kv_partner.at[t], partner_s.at[t], partner_r.at[t], partner)

        @pl.when(core == 0)
        def _():
            remote(kv_own.at[t], kv_x.at[t], x_s.at[t], x_r.at[t], x_to).start()

    loads[0].wait()
    loads[1].wait()
    for t in range(2):
        kv_own[t] = dot(emb[t * HALF : (t + 1) * HALF, :], wk[...]).astype(BF16)
    pl.semaphore_wait(barrier, len(friends))
    for t in range(2):
        kv_sends(t)
    loads[2].wait()
    for t in range(2):
        kv_own[2 + t] = dot(emb[t * HALF : (t + 1) * HALF, :], wv[...]).astype(BF16)
    for t in range(2, 4):
        kv_sends(t)

    loads[3].wait()
    for n in (6, 7, 8):
        loads[n].start()
    part = pl.ds(pl.multiple_of(core * BLOCK, BLOCK), BLOCK)
    for k in range(1, N_MP):
        here = attn_out.at[mp, part]
        send(here, here, ao_s.at[k - 1], ao_r.at[k - 1], mp_at(k))

    loads[4].wait()
    loads[9].wait()
    loads[10].wait()
    for t in range(2):
        rows = slice(t * HALF, (t + 1) * HALF)
        q = dot(emb[rows, :], wq[...])
        for h in range(HEADS):
            cols = slice(h * 64, (h + 1) * 64)
            qc[rows, cols] = (q[:, cols] + content_bias[h : h + 1, :]).astype(BF16)
            qp[rows, cols] = (q[:, cols] + position_bias[h : h + 1, :]).astype(BF16)

    loads[5].wait()
    loads[11].wait()
    rel[WIDTH:, :] = jnp.zeros((BLOCK, HALF), BF16)

    def rel_block(n, carry):
        for k in range(HALF // FINE):
            at = n * (HALF // FINE) + k
            sin_a, cos_a = basis[0, pl.ds(at, 1), :], basis[1, pl.ds(at, 1), :]
            sin_b, cos_b = basis[2], basis[3]
            rows = slice(k * FINE, (k + 1) * FINE)
            table[rows, : WIDTH // 2] = (sin_a * cos_b + cos_a * sin_b).astype(BF16)
            table[rows, WIDTH // 2 :] = (cos_a * cos_b - sin_a * sin_b).astype(BF16)
        rel[pl.ds(pl.multiple_of(n * HALF, HALF), HALF), :] = dot(table[...], wr[...]).astype(BF16)
        return carry

    lax.fori_loop(0, WIDTH // HALF, rel_block, 0)

    lanes = lax.broadcasted_iota(jnp.int32, (BLOCK, HALF), 1)
    row_at = lax.broadcasted_iota(jnp.int32, (BLOCK, BLOCK), 0)
    col_at = lax.broadcasted_iota(jnp.int32, (BLOCK, BLOCK), 1)

    def of_head(h):
        return (lanes >= h * 64) & (lanes < h * 64 + 64)

    def one_head(ref, rows, mine):
        values = ref[rows, :].astype(F32) * 0.125
        return jnp.where(mine, values, 0.0).astype(BF16)

    def relay(t):
        remote(kv_own.at[t], kv_same.at[t], same_s.at[t], same_r.at[t], forward).wait_recv()
        send(kv_same.at[t], kv_cross.at[t], cross_s.at[t], cross_r.at[t], partner)

        @pl.when(core == 1)
        def _():
            remote(kv_same.at[t], kv_x.at[t], x_s.at[t], x_r.at[t], x_to).start()

    for b in range(ROWS // BLOCK):
        rows = slice(b * BLOCK, (b + 1) * BLOCK)
        own = (b + 1) * BLOCK
        begin = ROWS - own
        width = WIDTH + BLOCK - begin

        keys = []
        for c in range(2):
            if own > c * HALF:
                keys.append((c, min(HALF, own - c * HALF)))
        outcome = None
        for h in range(HEADS):
            mine = of_head(h)
            near = dot_t(one_head(qp, rows, mine), rel[begin:, :])
            near = pltpu.roll(near, width - BLOCK + 1, 1, stride=1, stride_axis=0)
            pos_past[h, rows, :] = near[:, :ROWS]
            query = one_head(qc, rows, mine)
            content = [dot_t(query, kv_own[c, :n, :]) for c, n in keys]
            content = content[0] if len(content) == 1 else jnp.concatenate(content, axis=1)
            score = content + near[:, ROWS : ROWS + own]
            last = jnp.where(col_at <= row_at, score[:, own - BLOCK :], MASKED)
            score = last if own == BLOCK else jnp.concatenate([score[:, : own - BLOCK], last], axis=1)
            top = jnp.max(score, axis=-1, keepdims=True)
            weight = jnp.exp(score - top)
            top_own[h, rows, :] = top
            sum_own[h, rows, :] = jnp.sum(weight, axis=-1, keepdims=True)
            weight = weight.astype(BF16)
            total = None
            for c, n in keys:
                term = dot(weight[:, c * HALF : c * HALF + n], kv_own[2 + c, :n, :])
                total = term if total is None else total + term
            outcome = total if outcome is None else jnp.where(mine, total, outcome)
        out_own[rows, :] = outcome
        relay(b)

    for k in range(1, N_MP):
        there = lax.rem(mp + N_MP - k, N_MP)
        here = attn_out.at[there, part]
        remote(here, here, ao_s.at[k - 1], ao_r.at[k - 1], mp_at(k)).wait_recv()
        send(here, here, aof_s.at[k - 1], aof_r.at[k - 1], partner)

    for n in range(12, 19):
        loads[n].wait()
    spread = jnp.broadcast_to(targets[...].astype(F32), (BLOCK, ROWS))
    target_col[...] = jnp.transpose(spread)[:, :8]
    previous = pred_v[...]
    behind = jnp.broadcast_to(seg - previous, (HALF, HALF))
    has_memory = jnp.broadcast_to(previous, (BLOCK, ROWS)) >= 0
    use_cross = behind == 1 + 2 * core
    use_partner = behind == 2 * core - 1
    use_x = behind == 3 - 4 * core
    for t in range(4):
        remote(kv_own.at[t], kv_partner.at[t], partner_s.at[t], partner_r.at[t], partner).wait_recv()
        remote(kv_same.at[t], kv_cross.at[t], cross_s.at[t], cross_r.at[t], partner).wait_recv()
        remote(kv_same.at[t], kv_x.at[t], x_s.at[t], x_r.at[t], x_to).wait_recv()
        chosen = jnp.where(use_cross, kv_cross[t], kv_same[t])
        chosen = jnp.where(use_partner, kv_partner[t], chosen)
        kv_past[t] = jnp.where(use_x, kv_x[t], chosen)

    side = (mp_at(1), mp_at(N_MP - 1))
    source = (lax.rem(mp + N_MP - 1, N_MP), lax.rem(mp + 1, N_MP))
    across = lax.rem(mp + 2, N_MP)

    def pass_attended(b):
        for k in range(2):
            here = attended.at[source[k], b * BLOCK : (b + 1) * BLOCK]
            remote(here, here, att_s.at[k, b], att_r.at[k, b], side[k]).wait_recv()
            here = attended.at[source[k], b * BLOCK + k * PIECE : b * BLOCK + (k + 1) * PIECE]
            send(here, here, att_s.at[2 + k, b], att_r.at[2 + k, b], side[k])

    def attended_arrived(b):
        for k in range(2):
            here = attended.at[across, b * BLOCK + k * PIECE : b * BLOCK + (k + 1) * PIECE]
            remote(here, here, att_s.at[2 + k, b], att_r.at[2 + k, b], side[k]).wait_recv()

    for b in range(ROWS // BLOCK):
        rows = slice(b * BLOCK, (b + 1) * BLOCK)

        outcome = None
        for h in range(HEADS):
            mine = of_head(h)
            query = one_head(qc, rows, mine)
            score = jnp.concatenate([dot_t(query, kv_past[c]) for c in range(2)], axis=1)
            score = jnp.where(has_memory, score + pos_past[h, rows, :], MASKED)
            before = top_own[h, rows, :]
            top = jnp.maximum(before, jnp.max(score, axis=-1, keepdims=True))
            weight = jnp.exp(score - top)
            fade = jnp.exp(before - top)
            total = sum_own[h, rows, :] * fade + jnp.sum(weight, axis=-1, keepdims=True)
            weight = weight.astype(BF16)
            past = dot(weight[:, :HALF], kv_past[2]) + dot(weight[:, HALF:], kv_past[3])
            done = (out_own[rows, :] * fade + past) / total
            outcome = done if outcome is None else jnp.where(mine, done, outcome)
        attended[mp, rows, :] = outcome.astype(BF16)
        here = attended.at[mp, rows]
        for k in range(2):
            send(here, here, att_s.at[k, b], att_r.at[k, b], side[k])
        if b > 0:
            pass_attended(b - 1)

    for k in range(1, N_MP):
        there = lax.rem(mp + N_MP - k, N_MP)
        other = pl.ds(pl.multiple_of((1 - core) * BLOCK, BLOCK), BLOCK)
        here = attn_out.at[there, other]
        remote(here, here, aof_s.at[k - 1], aof_r.at[k - 1], partner).wait_recv()
    loads[6].wait()
    loads[7].wait()
    loads[8].wait()

    part_rows = (slice(0, PIECE // 2), slice(PIECE // 2, PIECE))

    def reduce_copy(half, n):
        k = n % 2
        if n < 2:
            src = rs_send.at[half, source[1 - k], part_rows[1 - k]]
        elif n < 4:
            src = rs_pass.at[half, k]
        else:
            src = rs_send.at[half, across, part_rows[k]]
        return remote(src, rs_recv.at[half, n], rs_s.at[n, half], rs_r.at[n, half], side[k])

    def start_reduce(half, n):
        copy = reduce_copy(half, n)
        copy.start()
        pending.append(copy)

    def pass_reduce(half):
        for k in range(2):
            reduce_copy(half, 4 + k).wait_recv()
            mine = rs_send[half, source[1 - k], part_rows[k]].astype(F32)
            rs_pass[half, k] = (mine + rs_recv[half, 4 + k].astype(F32)).astype(BF16)
            start_reduce(half, 2 + k)

    for half in range(2):
        rows = slice(half * HALF, (half + 1) * HALF)
        if half == 1:
            attended_arrived(2)
            attended_arrived(3)
        else:
            attended_arrived(0)
            attended_arrived(1)
        total = emb[rows, :].astype(F32)
        head_sum = None
        for g in range(N_MP):
            term = dot(attended[g, rows, :], attn_out[g]).astype(BF16).astype(F32)
            head_sum = term if head_sum is None else head_sum + term
        first = normalize(total + head_sum, attn_gain[...], attn_shift[...]).astype(BF16)
        first_out[rows, :] = first
        if half == 0:
            pass_attended(3)
        units[...] = jnp.maximum(dot(first, wup[...]) + up_bias[...], 0.0).astype(BF16)
        if half == 1:
            pass_reduce(0)
        terms = dot(units[...], wdown[...]).astype(BF16)
        for d in range(N_MP):
            rs_send[half, d] = terms[d * PIECE : (d + 1) * PIECE, :]
        for n in (4, 5, 0, 1):
            start_reduce(half, n)

    def second_copy(half, n):
        k = n % 2
        if n < 2:
            here = second.at[half, mp]
        else:
            here = second.at[half, source[k], part_rows[k]]
        return remote(here, here, ag_s.at[n, half], ag_r.at[n, half], side[k])

    def start_second(half, n):
        copy = second_copy(half, n)
        copy.start()
        pending.append(copy)

    def pass_second(half):
        for k in range(2):
            here = second.at[half, source[k]]
            remote(here, here, ag_s.at[k, half], ag_r.at[k, half], side[k]).wait_recv()
            start_second(half, 2 + k)

    def second_arrived(half):
        for k in range(2):
            here = second.at[half, across, part_rows[k]]
            remote(here, here, ag_s.at[2 + k, half], ag_r.at[2 + k, half], side[k]).wait_recv()

    def finish_reduce(half):
        for n in range(4):
            reduce_copy(half, n).wait_recv()
        for k in range(2):
            total = rs_send[half, mp, part_rows[k]].astype(F32)
            total = total + rs_recv[half, 1 - k].astype(F32) + rs_recv[half, 2 + k].astype(F32)
            start = half * HALF + mp * PIECE + k * (PIECE // 2)
            at = pl.ds(pl.multiple_of(start, PIECE // 2), PIECE // 2)
            total = first_out[at, :].astype(F32) + total + down_bias[...]
            total = normalize(total, ffn_gain[...], ffn_shift[...]).astype(BF16)
            second[half, mp, part_rows[k]] = total
        for n in range(2):
            start_second(half, n)

    finish_reduce(0)
    pass_reduce(1)
    pass_second(0)
    finish_reduce(1)

    tile = 512
    n_words = wvocab_h.shape[1]
    for half in range(2):
        rows = slice(half * HALF, (half + 1) * HALF)
        second_arrived(half)
        states = jnp.concatenate([second[half, d] for d in range(N_MP)], axis=0)
        wanted = target_col[rows, 0:1].astype(jnp.int32) - mp * n_words
        words = lax.broadcasted_iota(jnp.int32, (HALF, tile), 1)

        def vocab_tile(n, carry, states=states, wanted=wanted, words=words):
            top, total, picked = carry
            at = pl.multiple_of(n * tile, tile)
            logits = dot(states, wvocab[:, pl.ds(at, tile)])
            new_top = jnp.maximum(top, jnp.max(logits, axis=1, keepdims=True))
            total = total * jnp.exp(top - new_top)
            total = total + jnp.sum(jnp.exp(logits - new_top), axis=1, keepdims=True)
            hit = jnp.where(words == wanted - at, logits, 0.0)
            return new_top, total, picked + jnp.sum(hit, axis=1, keepdims=True)

        zero = jnp.zeros((HALF, 1), F32)
        found = (jnp.full((HALF, 1), -jnp.inf, F32), zero, zero)
        found = lax.fori_loop(0, 2, vocab_tile, found)
        if half == 0:
            pass_second(1)
        top, total, picked = lax.fori_loop(2, n_words // tile, vocab_tile, found)
        lane = lax.broadcasted_iota(jnp.int32, (HALF, BLOCK), 1)
        packed = jnp.where(lane == 0, top, jnp.where(lane == 1, total, picked))
        stats[mp, :, rows] = jnp.transpose(packed)[:8, :]

    for k in range(1, N_MP):
        here = stats.at[mp]
        send(here, here, st_s.at[k - 1], st_r.at[k - 1], mp_at(k))
    for k in range(1, N_MP):
        there = lax.rem(mp + N_MP - k, N_MP)
        here = stats.at[there]
        remote(here, here, st_s.at[k - 1], st_r.at[k - 1], mp_at(k)).wait_recv()
    top = stats[0, 0:1, :]
    for g in range(1, N_MP):
        top = jnp.maximum(top, stats[g, 0:1, :])
    total, picked = None, None
    for g in range(N_MP):
        term = stats[g, 1:2, :] * jnp.exp(stats[g, 0:1, :] - top)
        total = term if total is None else total + term
        picked = stats[g, 2:3, :] if picked is None else picked + stats[g, 2:3, :]
    position = lax.broadcasted_iota(jnp.int32, (1, ROWS), 1)
    tokens = jnp.where(position < jnp.broadcast_to(valid_v[...], (1, ROWS)), picked - (top + jnp.log(total)), 0.0)
    token_o[...] = tokens

    slot = lax.broadcasted_iota(jnp.int32, (8, BLOCK), 1) == jnp.broadcast_to(doc_v[...], (8, BLOCK))
    line = lax.broadcasted_iota(jnp.int32, (8, BLOCK), 0)
    used = valid_v[...].astype(F32)
    share = jnp.sum(tokens, axis=1, keepdims=True)
    doc_a[0] = jnp.where(slot, jnp.where(line == 0, share, jnp.where(line == 1, used, 0.0)), 0.0)
    for k in range(1, group):
        send(doc_a.at[0], doc_a.at[k], da_s.at[k - 1], da_r.at[k - 1], group_at(k))
    for k in range(1, group):
        remote(doc_a.at[0], doc_a.at[k], da_s.at[k - 1], da_r.at[k - 1], group_at(k)).wait_recv()
    doc_b[0] = jnp.sum(doc_a[...], axis=0)
    for k in range(1, n_z):
        send(doc_b.at[0], doc_b.at[k], db_s.at[k - 1], db_r.at[k - 1], z_at(k))
    for k in range(1, n_z):
        remote(doc_b.at[0], doc_b.at[k], db_s.at[k - 1], db_r.at[k - 1], z_at(k)).wait_recv()
    docs = jnp.sum(doc_b[...], axis=0)
    doc_o[...] = docs[0:1, :] / docs[1:2, :]

    for copy in pending:
        copy.wait_send()
    for t in range(4):
        remote(kv_own.at[t], kv_x.at[t], x_s.at[t], x_r.at[t], x_to).wait_send()


def hand_over(token_i, doc_i, token_o, doc_o):
    token_o[...] = token_i[...]
    doc_o[...] = doc_i[:, : doc_o.shape[1]]


def angle_basis():
    frequency = 10000.0 ** (-np.arange(0, WIDTH, 2, dtype=np.float64) / WIDTH)
    coarse = (WIDTH // FINE - 1 - np.arange(WIDTH // FINE))[:, None] * FINE * frequency[None, :]
    fine = (FINE - 1 - np.arange(FINE))[:, None] * frequency[None, :]
    return np.stack([np.sin(coarse), np.cos(coarse), np.sin(fine), np.cos(fine)]).astype(np.float32)


def on_device(
    n_seg,
    embedded,
    targets,
    pred_device,
    doc_ids,
    valid_rows,
    w_query,
    w_key,
    w_value,
    w_rel,
    content_bias,
    position_bias,
    attn_out,
    attn_gain,
    attn_shift,
    w_up,
    up_bias,
    w_down,
    down_bias,
    ffn_gain,
    ffn_shift,
    w_vocab,
):
    vmem = pl.BlockSpec(memory_space=pltpu.VMEM)
    hbm = pl.BlockSpec(memory_space=pltpu.HBM)
    dma = pltpu.SemaphoreType.DMA
    words = w_vocab.shape[1]
    n_z = n_seg // (2 * N_X)
    kv = pltpu.VMEM((4, HALF, HALF), BF16)
    weight = pltpu.VMEM((WIDTH, HALF), BF16)
    column = pltpu.VMEM((HEADS, ROWS, 1), F32)
    vector = pltpu.VMEM((1, WIDTH), F32)
    scratch = [
        pltpu.VMEM((HEADS, 64), F32),
        pltpu.VMEM((HEADS, 64), F32),
        pltpu.VMEM((4, FINE, WIDTH // 2), F32),
        pltpu.VMEM((1, ROWS), jnp.int32),
        vector,
        vector,
        vector,
        vector,
        vector,
        vector,
        pltpu.VMEM((ROWS, WIDTH), BF16),
        weight,
        weight,
        weight,
        weight,
        pltpu.VMEM((N_MP, HALF, WIDTH), BF16),
        pltpu.VMEM((WIDTH, WIDTH), BF16),
        pltpu.VMEM((WIDTH, WIDTH), BF16),
        pltpu.VMEM((WIDTH, words), BF16),
        pltpu.VMEM((HALF, WIDTH), BF16),
        pltpu.VMEM((WIDTH + BLOCK, HALF), BF16),
        pltpu.VMEM((ROWS, HALF), BF16),
        pltpu.VMEM((ROWS, HALF), BF16),
        kv,
        kv,
        kv,
        kv,
        kv,
        kv,
        pltpu.VMEM((HEADS, ROWS, ROWS), F32),
        column,
        column,
        pltpu.VMEM((ROWS, HALF), F32),
        pltpu.VMEM((N_MP, ROWS, HALF), BF16),
        pltpu.VMEM((ROWS, WIDTH), BF16),
        pltpu.VMEM((HALF, WIDTH), BF16),
        pltpu.VMEM((2, N_MP, PIECE, WIDTH), BF16),
        pltpu.VMEM((2, 6, PIECE // 2, WIDTH), BF16),
        pltpu.VMEM((2, 2, PIECE // 2, WIDTH), BF16),
        pltpu.VMEM((2, N_MP, PIECE, WIDTH), BF16),
        pltpu.VMEM((ROWS, 8), F32),
        pltpu.VMEM((N_MP, 8, ROWS), F32),
        pltpu.VMEM((2 * N_X, 8, BLOCK), F32),
        pltpu.VMEM((n_z, 8, BLOCK), F32),
        dma((19,)),
    ]
    scratch += [dma((4,))] * 8
    scratch += [dma((N_MP - 1,))] * 4
    scratch += [dma((4, 4))] * 2
    scratch += [dma((6, 2))] * 2
    scratch += [dma((4, 2))] * 2
    scratch += [dma((N_MP - 1,))] * 2
    scratch += [dma((2 * N_X - 1,))] * 2
    scratch += [dma((n_z - 1,))] * 2
    token_terms, docs = pl.pallas_call(
        functools.partial(kernel, n_seg),
        out_shape=(
            jax.ShapeDtypeStruct((1, ROWS), F32),
            jax.ShapeDtypeStruct((1, BLOCK), F32),
        ),
        in_specs=[vmem] * 3 + [hbm] * 19,
        out_specs=(vmem, vmem),
        scratch_shapes=scratch,
        compiler_params=pltpu.CompilerParams(
            collective_id=0, has_side_effects=True, vmem_limit_bytes=60 * 1024 * 1024
        ),
        name="layer",
    )(
        pred_device.reshape(1, 1),
        doc_ids.reshape(1, 1),
        valid_rows.reshape(1, 1),
        content_bias,
        position_bias,
        jnp.asarray(angle_basis()),
        targets.reshape(1, ROWS),
        attn_gain.reshape(1, WIDTH),
        attn_shift.reshape(1, WIDTH),
        up_bias.reshape(1, WIDTH),
        down_bias.reshape(1, WIDTH),
        ffn_gain.reshape(1, WIDTH),
        ffn_shift.reshape(1, WIDTH),
        embedded,
        w_query,
        w_key,
        w_value,
        w_rel,
        attn_out,
        w_up,
        w_down,
        w_vocab,
    )
    doc_slots = n_seg // 4
    token_terms, docs = pl.pallas_call(
        hand_over,
        out_shape=(
            jax.ShapeDtypeStruct((1, ROWS), F32),
            jax.ShapeDtypeStruct((1, doc_slots), F32),
        ),
        in_specs=[vmem, vmem],
        out_specs=(vmem, vmem),
        name="results",
    )(token_terms, docs)
    return token_terms.reshape(ROWS), docs.reshape(doc_slots)


def solution(mesh):
    return jax.shard_map(
        functools.partial(on_device, mesh.shape["seg"]),
        mesh=mesh,
        in_specs=(
            P("seg", None),
            P("seg"),
            P("seg"),
            P("seg"),
            P("seg"),
            P(None, "mp"),
            P(None, "mp"),
            P(None, "mp"),
            P(None, "mp"),
            P("mp", None),
            P("mp", None),
            P("mp", None),
            P(),
            P(),
            P(None, "mp"),
            P("mp"),
            P("mp", None),
            P(),
            P(),
            P(),
            P(None, "mp"),
        ),
        out_specs=(P("seg"), P()),
        check_vma=False,
    )
```

```python
import functools

import jax
import jax.numpy as jnp
import numpy as np
from jax import lax
from jax.experimental import pallas as pl
from jax.experimental.pallas import tpu as pltpu
from jax.sharding import PartitionSpec as P

EPSILON = 1e-05
MESH = pl.DeviceIdType.MESH
F32, BF16 = jnp.float32, jnp.bfloat16
N_X = 4
N_MP = 4
HEADS = 4
ROWS = 512
WIDTH = 1024
BLOCK = 128
HALF = 256
PIECE = 32
FINE = 32
MASKED = -1e30


def normalize(values, gain, shift):
    centre = values - jnp.mean(values, axis=-1, keepdims=True)
    spread = jnp.mean(centre * centre, axis=-1, keepdims=True)
    return centre * lax.rsqrt(spread + EPSILON) * gain + shift


def dot(a, b):
    return jnp.dot(a, b, preferred_element_type=F32)


def dot_t(a, b):
    return lax.dot_general(a, b, (((1,), (1,)), ((), ())), preferred_element_type=F32)


def kernel(
    n_seg,
    pred_v,
    doc_v,
    valid_v,
    content_bias_h,
    position_bias_h,
    basis_h,
    targets_h,
    attn_gain_h,
    attn_shift_h,
    up_bias_h,
    down_bias_h,
    ffn_gain_h,
    ffn_shift_h,
    embedded_h,
    wq_h,
    wk_h,
    wv_h,
    wr_h,
    attn_out_h,
    wup_h,
    wdown_h,
    wvocab_h,
    token_o,
    doc_o,
    content_bias,
    position_bias,
    basis,
    targets,
    attn_gain,
    attn_shift,
    up_bias,
    down_bias,
    ffn_gain,
    ffn_shift,
    emb,
    wq,
    wk,
    wv,
    wr,
    attn_out,
    wup,
    wdown,
    wvocab,
    table,
    rel,
    qc,
    qp,
    kv_own,
    kv_same,
    kv_partner,
    kv_cross,
    kv_x,
    kv_past,
    pos_past,
    weights,
    top_own,
    sum_own,
    out_own,
    attended,
    first_out,
    units,
    rs_send,
    rs_recv,
    second,
    target_col,
    stats,
    doc_a,
    doc_b,
    load_sem,
    same_s,
    same_r,
    partner_s,
    partner_r,
    cross_s,
    cross_r,
    x_s,
    x_r,
    ao_s,
    ao_r,
    aof_s,
    aof_r,
    att_s,
    att_r,
    rs_s,
    rs_r,
    ag_s,
    ag_r,
    st_s,
    st_r,
    da_s,
    da_r,
    db_s,
    db_r,
):
    seg = lax.axis_index("seg")
    mp = lax.axis_index("mp")
    core = lax.rem(seg, 2)
    chip = lax.div(seg, 2)
    n_chip = n_seg // 2
    group = 2 * N_X
    n_z = n_seg // group
    in_group = lax.rem(seg, group)
    z = lax.div(seg, group)

    def chip_at(step, c):
        return (lax.rem(chip + step + n_chip, n_chip) * 2 + c, mp)

    partner = (chip * 2 + 1 - core, mp)
    forward = chip_at(1, core)
    backward = chip_at(-1, core)

    def mp_at(k):
        return (seg, lax.rem(mp + k, N_MP))

    def group_at(k):
        return (z * group + lax.rem(in_group + k, group), mp)

    def z_at(k):
        return (lax.rem(z + k, n_z) * group + in_group, mp)

    x_to = (lax.rem(chip + n_chip + 2 * core - 1, n_chip) * 2 + 1 - core, mp)

    pending = []

    def remote(src, dst, s_sem, r_sem, device):
        return pltpu.make_async_remote_copy(
            src_ref=src,
            dst_ref=dst,
            send_sem=s_sem,
            recv_sem=r_sem,
            device_id=device,
            device_id_type=MESH,
        )

    def send(*args):
        copy = remote(*args)
        copy.start()
        pending.append(copy)

    sources = (
        (embedded_h, emb),
        (wk_h, wk),
        (wv_h, wv),
        (attn_out_h, attn_out.at[mp]),
        (wq_h, wq),
        (wr_h, wr),
        (wup_h, wup),
        (wdown_h, wdown),
        (wvocab_h, wvocab),
        (content_bias_h, content_bias),
        (position_bias_h, position_bias),
        (basis_h, basis),
        (targets_h, targets),
        (attn_gain_h, attn_gain),
        (attn_shift_h, attn_shift),
        (up_bias_h, up_bias),
        (down_bias_h, down_bias),
        (ffn_gain_h, ffn_gain),
        (ffn_shift_h, ffn_shift),
    )
    loads = [pltpu.make_async_copy(src, dst, load_sem.at[n]) for n, (src, dst) in enumerate(sources)]
    for n in (0, 1, 2, 4, 9, 10, 11, 5, 3, *range(12, 19)):
        loads[n].start()

    barrier = pltpu.get_barrier_semaphore()
    friends = [partner, forward, backward, x_to]
    friends += [mp_at(k) for k in range(1, N_MP)]
    friends += [group_at(k) for k in range(1, group)]
    friends += [z_at(k) for k in range(1, n_z)]
    for friend in friends:
        pl.semaphore_signal(barrier, inc=1, device_id=friend, device_id_type=MESH)

    def kv_sends(t):
        send(kv_own.at[t], kv_same.at[t], same_s.at[t], same_r.at[t], forward)
        send(kv_own.at[t], kv_partner.at[t], partner_s.at[t], partner_r.at[t], partner)

        @pl.when(core == 0)
        def _():
            remote(kv_own.at[t], kv_x.at[t], x_s.at[t], x_r.at[t], x_to).start()

    loads[0].wait()
    loads[1].wait()
    for t in range(2):
        kv_own[t] = dot(emb[t * HALF : (t + 1) * HALF, :], wk[...]).astype(BF16)
    pl.semaphore_wait(barrier, len(friends))
    for t in range(2):
        kv_sends(t)
    loads[2].wait()
    for t in range(2):
        kv_own[2 + t] = dot(emb[t * HALF : (t + 1) * HALF, :], wv[...]).astype(BF16)
    for t in range(2, 4):
        kv_sends(t)

    loads[3].wait()
    for n in (6, 7, 8):
        loads[n].start()
    part = pl.ds(pl.multiple_of(core * BLOCK, BLOCK), BLOCK)
    for k in range(1, N_MP):
        here = attn_out.at[mp, part]
        send(here, here, ao_s.at[k - 1], ao_r.at[k - 1], mp_at(k))

    loads[4].wait()
    loads[9].wait()
    loads[10].wait()
    for t in range(2):
        rows = slice(t * HALF, (t + 1) * HALF)
        q = dot(emb[rows, :], wq[...])
        for h in range(HEADS):
            cols = slice(h * 64, (h + 1) * 64)
            qc[rows, cols] = (q[:, cols] + content_bias[h : h + 1, :]).astype(BF16)
            qp[rows, cols] = (q[:, cols] + position_bias[h : h + 1, :]).astype(BF16)

    loads[5].wait()
    loads[11].wait()
    rel[WIDTH:, :] = jnp.zeros((BLOCK, HALF), BF16)

    def rel_block(n, carry):
        for k in range(HALF // FINE):
            at = n * (HALF // FINE) + k
            sin_a, cos_a = basis[0, pl.ds(at, 1), :], basis[1, pl.ds(at, 1), :]
            sin_b, cos_b = basis[2], basis[3]
            rows = slice(k * FINE, (k + 1) * FINE)
            table[rows, : WIDTH // 2] = (sin_a * cos_b + cos_a * sin_b).astype(BF16)
            table[rows, WIDTH // 2 :] = (cos_a * cos_b - sin_a * sin_b).astype(BF16)
        rel[pl.ds(pl.multiple_of(n * HALF, HALF), HALF), :] = dot(table[...], wr[...]).astype(BF16)
        return carry

    lax.fori_loop(0, WIDTH // HALF, rel_block, 0)

    lanes = lax.broadcasted_iota(jnp.int32, (BLOCK, HALF), 1)
    row_at = lax.broadcasted_iota(jnp.int32, (BLOCK, BLOCK), 0)
    col_at = lax.broadcasted_iota(jnp.int32, (BLOCK, BLOCK), 1)

    def of_head(h):
        return (lanes >= h * 64) & (lanes < h * 64 + 64)

    def one_head(ref, rows, mine):
        values = ref[rows, :].astype(F32) * 0.125
        return jnp.where(mine, values, 0.0).astype(BF16)

    def relay(t):
        remote(kv_own.at[t], kv_same.at[t], same_s.at[t], same_r.at[t], forward).wait_recv()
        send(kv_same.at[t], kv_cross.at[t], cross_s.at[t], cross_r.at[t], partner)

        @pl.when(core == 1)
        def _():
            remote(kv_same.at[t], kv_x.at[t], x_s.at[t], x_r.at[t], x_to).start()

    for b in range(ROWS // BLOCK):
        rows = slice(b * BLOCK, (b + 1) * BLOCK)
        own = (b + 1) * BLOCK
        begin = ROWS - own
        width = WIDTH + BLOCK - begin

        keys = []
        for c in range(2):
            if own > c * HALF:
                keys.append((c, min(HALF, own - c * HALF)))
        outcome = None
        for h in range(HEADS):
            mine = of_head(h)
            near = dot_t(one_head(qp, rows, mine), rel[begin:, :])
            near = pltpu.roll(near, width - BLOCK + 1, 1, stride=1, stride_axis=0)
            pos_past[h, rows, :] = near[:, :ROWS]
            query = one_head(qc, rows, mine)
            content = [dot_t(query, kv_own[c, :n, :]) for c, n in keys]
            content = content[0] if len(content) == 1 else jnp.concatenate(content, axis=1)
            score = content + near[:, ROWS : ROWS + own]
            last = jnp.where(col_at <= row_at, score[:, own - BLOCK :], MASKED)
            score = last if own == BLOCK else jnp.concatenate([score[:, : own - BLOCK], last], axis=1)
            top = jnp.max(score, axis=-1, keepdims=True)
            weight = jnp.exp(score - top)
            top_own[h, rows, :] = top
            sum_own[h, rows, :] = jnp.sum(weight, axis=-1, keepdims=True)
            weight = weight.astype(BF16)
            total = None
            for c, n in keys:
                term = dot(weight[:, c * HALF : c * HALF + n], kv_own[2 + c, :n, :])
                total = term if total is None else total + term
            outcome = total if outcome is None else jnp.where(mine, total, outcome)
        out_own[rows, :] = outcome
        relay(b)

    for k in range(1, N_MP):
        there = lax.rem(mp + N_MP - k, N_MP)
        here = attn_out.at[there, part]
        remote(here, here, ao_s.at[k - 1], ao_r.at[k - 1], mp_at(k)).wait_recv()
        send(here, here, aof_s.at[k - 1], aof_r.at[k - 1], partner)

    for n in range(12, 19):
        loads[n].wait()
    spread = jnp.broadcast_to(targets[...].astype(F32), (BLOCK, ROWS))
    target_col[...] = jnp.transpose(spread)[:, :8]
    previous = pred_v[...]
    behind = jnp.broadcast_to(seg - previous, (HALF, HALF))
    has_memory = jnp.broadcast_to(previous, (BLOCK, ROWS)) >= 0
    use_cross = behind == 1 + 2 * core
    use_partner = behind == 2 * core - 1
    use_x = behind == 3 - 4 * core

    def choose(t):
        remote(kv_own.at[t], kv_partner.at[t], partner_s.at[t], partner_r.at[t], partner).wait_recv()
        remote(kv_same.at[t], kv_cross.at[t], cross_s.at[t], cross_r.at[t], partner).wait_recv()
        remote(kv_same.at[t], kv_x.at[t], x_s.at[t], x_r.at[t], x_to).wait_recv()
        chosen = jnp.where(use_cross, kv_cross[t], kv_same[t])
        chosen = jnp.where(use_partner, kv_partner[t], chosen)
        kv_past[t] = jnp.where(use_x, kv_x[t], chosen)

    def origin(k):
        return lax.rem(mp + N_MP - k, N_MP)

    def attended_copy(b, k, owner):
        here = attended.at[owner, b * BLOCK : (b + 1) * BLOCK]
        return remote(here, here, att_s.at[k - 1, b], att_r.at[k - 1, b], mp_at(k))

    def reduce_copy(b, k):
        src = rs_send.at[b, lax.rem(mp + k, N_MP)]
        return remote(src, rs_recv.at[b, k - 1], rs_s.at[k - 1, b], rs_r.at[k - 1, b], mp_at(k))

    def second_copy(b, k, owner):
        here = second.at[b, owner]
        return remote(here, here, ag_s.at[k - 1, b], ag_r.at[k - 1, b], mp_at(k))

    def begin(copy):
        copy.start()
        pending.append(copy)

    def weigh(b):
        rows = slice(b * BLOCK, (b + 1) * BLOCK)
        for h in range(HEADS):
            query = one_head(qc, rows, of_head(h))
            score = jnp.concatenate([dot_t(query, kv_past[c]) for c in range(2)], axis=1)
            score = jnp.where(has_memory, score + pos_past[h, rows, :], MASKED)
            before = top_own[h, rows, :]
            top = jnp.maximum(before, jnp.max(score, axis=-1, keepdims=True))
            weight = jnp.exp(score - top)
            fade = jnp.exp(before - top)
            sum_own[h, rows, :] = sum_own[h, rows, :] * fade + jnp.sum(weight, axis=-1, keepdims=True)
            top_own[h, rows, :] = fade
            weights[h, rows, :] = weight.astype(BF16)

    def attend(b):
        rows = slice(b * BLOCK, (b + 1) * BLOCK)
        outcome = None
        for h in range(HEADS):
            past = dot(weights[h, rows, :HALF], kv_past[2]) + dot(weights[h, rows, HALF:], kv_past[3])
            done = (out_own[rows, :] * top_own[h, rows, :] + past) / sum_own[h, rows, :]
            outcome = done if outcome is None else jnp.where(of_head(h), done, outcome)
        attended[mp, rows, :] = outcome.astype(BF16)
        for k in (2, 1, 3):
            begin(attended_copy(b, k, mp))

    def feed(b):
        rows = slice(b * BLOCK, (b + 1) * BLOCK)
        for k in range(1, N_MP):
            attended_copy(b, k, origin(k)).wait_recv()
        head_sum = None
        for g in range(N_MP):
            term = dot(attended[g, rows, :], attn_out[g]).astype(BF16).astype(F32)
            head_sum = term if head_sum is None else head_sum + term
        total = emb[rows, :].astype(F32) + head_sum
        first = normalize(total, attn_gain[...], attn_shift[...]).astype(BF16)
        first_out[rows, :] = first
        units[...] = jnp.maximum(dot(first, wup[...]) + up_bias[...], 0.0).astype(BF16)
        terms = dot(units[...], wdown[...]).astype(BF16)
        for d in range(N_MP):
            rs_send[b, d] = terms[d * PIECE : (d + 1) * PIECE, :]
        for k in (2, 1, 3):
            begin(reduce_copy(b, k))

    def finish_reduce(b):
        total = rs_send[b, mp].astype(F32)
        for k in range(1, N_MP):
            reduce_copy(b, k).wait_recv()
            total = total + rs_recv[b, k - 1].astype(F32)
        at = pl.ds(pl.multiple_of(b * BLOCK + mp * PIECE, PIECE), PIECE)
        total = first_out[at, :].astype(F32) + total + down_bias[...]
        second[b, mp] = normalize(total, ffn_gain[...], ffn_shift[...]).astype(BF16)
        for k in (2, 1, 3):
            begin(second_copy(b, k, mp))

    def second_arrived(b):
        for k in range(1, N_MP):
            second_copy(b, k, origin(k)).wait_recv()

    choose(0)
    choose(1)
    weigh(0)
    weigh(1)
    choose(2)
    choose(3)
    attend(0)
    attend(1)
    weigh(2)
    attend(2)
    for k in range(1, N_MP):
        there = lax.rem(mp + N_MP - k, N_MP)
        other = pl.ds(pl.multiple_of((1 - core) * BLOCK, BLOCK), BLOCK)
        here = attn_out.at[there, other]
        remote(here, here, aof_s.at[k - 1], aof_r.at[k - 1], partner).wait_recv()
    for n in (6, 7, 8):
        loads[n].wait()
    weigh(3)
    feed(0)
    attend(3)
    feed(1)
    feed(2)
    finish_reduce(0)
    feed(3)
    finish_reduce(1)
    finish_reduce(2)

    tile = 512
    n_words = wvocab_h.shape[1]
    for blocks in ((0, 1), (2,), (3,)):
        count = len(blocks) * BLOCK
        rows = slice(blocks[0] * BLOCK, blocks[0] * BLOCK + count)
        for b in blocks:
            second_arrived(b)
        states = [second[b, d] for b in blocks for d in range(N_MP)]
        states = jnp.concatenate(states, axis=0)
        wanted = target_col[rows, 0:1].astype(jnp.int32) - mp * n_words
        words = lax.broadcasted_iota(jnp.int32, (count, tile), 1)

        def vocab_tile(n, carry, states=states, wanted=wanted, words=words):
            top, total, picked = carry
            at = pl.multiple_of(n * tile, tile)
            logits = dot(states, wvocab[:, pl.ds(at, tile)])
            new_top = jnp.maximum(top, jnp.max(logits, axis=1, keepdims=True))
            total = total * jnp.exp(top - new_top)
            total = total + jnp.sum(jnp.exp(logits - new_top), axis=1, keepdims=True)
            hit = jnp.where(words == wanted - at, logits, 0.0)
            return new_top, total, picked + jnp.sum(hit, axis=1, keepdims=True)

        zero = jnp.zeros((count, 1), F32)
        found = (jnp.full((count, 1), -jnp.inf, F32), zero, zero)
        found = lax.fori_loop(0, 2, vocab_tile, found)
        if blocks[0] == 0:
            finish_reduce(3)
        top, total, picked = lax.fori_loop(2, n_words // tile, vocab_tile, found)
        lane = lax.broadcasted_iota(jnp.int32, (count, BLOCK), 1)
        packed = jnp.where(lane == 0, top, jnp.where(lane == 1, total, picked))
        stats[mp, :, rows] = jnp.transpose(packed)[:8, :]

    for k in range(1, N_MP):
        here = stats.at[mp]
        send(here, here, st_s.at[k - 1], st_r.at[k - 1], mp_at(k))
    for k in range(1, N_MP):
        there = lax.rem(mp + N_MP - k, N_MP)
        here = stats.at[there]
        remote(here, here, st_s.at[k - 1], st_r.at[k - 1], mp_at(k)).wait_recv()
    top = stats[0, 0:1, :]
    for g in range(1, N_MP):
        top = jnp.maximum(top, stats[g, 0:1, :])
    total, picked = None, None
    for g in range(N_MP):
        term = stats[g, 1:2, :] * jnp.exp(stats[g, 0:1, :] - top)
        total = term if total is None else total + term
        picked = stats[g, 2:3, :] if picked is None else picked + stats[g, 2:3, :]
    position = lax.broadcasted_iota(jnp.int32, (1, ROWS), 1)
    tokens = jnp.where(position < jnp.broadcast_to(valid_v[...], (1, ROWS)), picked - (top + jnp.log(total)), 0.0)
    token_o[...] = tokens

    slot = lax.broadcasted_iota(jnp.int32, (8, BLOCK), 1) == jnp.broadcast_to(doc_v[...], (8, BLOCK))
    line = lax.broadcasted_iota(jnp.int32, (8, BLOCK), 0)
    used = valid_v[...].astype(F32)
    share = jnp.sum(tokens, axis=1, keepdims=True)
    doc_a[0] = jnp.where(slot, jnp.where(line == 0, share, jnp.where(line == 1, used, 0.0)), 0.0)
    for k in range(1, group):
        send(doc_a.at[0], doc_a.at[k], da_s.at[k - 1], da_r.at[k - 1], group_at(k))
    for k in range(1, group):
        remote(doc_a.at[0], doc_a.at[k], da_s.at[k - 1], da_r.at[k - 1], group_at(k)).wait_recv()
    doc_b[0] = jnp.sum(doc_a[...], axis=0)
    earlier = list(pending)
    for k in range(1, n_z):
        send(doc_b.at[0], doc_b.at[k], db_s.at[k - 1], db_r.at[k - 1], z_at(k))
    for copy in earlier:
        copy.wait_send()
    for t in range(4):
        remote(kv_own.at[t], kv_x.at[t], x_s.at[t], x_r.at[t], x_to).wait_send()
    for k in range(1, n_z):
        remote(doc_b.at[0], doc_b.at[k], db_s.at[k - 1], db_r.at[k - 1], z_at(k)).wait_recv()
    docs = jnp.sum(doc_b[...], axis=0)
    doc_o[...] = docs[0:1, :] / docs[1:2, :]
    for copy in pending[len(earlier) :]:
        copy.wait_send()


def hand_over(token_i, doc_i, token_o, doc_o):
    token_o[...] = token_i[...]
    doc_o[...] = doc_i[:, : doc_o.shape[1]]


def angle_basis():
    frequency = 10000.0 ** (-np.arange(0, WIDTH, 2, dtype=np.float64) / WIDTH)
    coarse = (WIDTH // FINE - 1 - np.arange(WIDTH // FINE))[:, None] * FINE * frequency[None, :]
    fine = (FINE - 1 - np.arange(FINE))[:, None] * frequency[None, :]
    return np.stack([np.sin(coarse), np.cos(coarse), np.sin(fine), np.cos(fine)]).astype(np.float32)


def on_device(
    n_seg,
    embedded,
    targets,
    pred_device,
    doc_ids,
    valid_rows,
    w_query,
    w_key,
    w_value,
    w_rel,
    content_bias,
    position_bias,
    attn_out,
    attn_gain,
    attn_shift,
    w_up,
    up_bias,
    w_down,
    down_bias,
    ffn_gain,
    ffn_shift,
    w_vocab,
):
    vmem = pl.BlockSpec(memory_space=pltpu.VMEM)
    hbm = pl.BlockSpec(memory_space=pltpu.HBM)
    dma = pltpu.SemaphoreType.DMA
    words = w_vocab.shape[1]
    n_z = n_seg // (2 * N_X)
    kv = pltpu.VMEM((4, HALF, HALF), BF16)
    weight = pltpu.VMEM((WIDTH, HALF), BF16)
    column = pltpu.VMEM((HEADS, ROWS, 1), F32)
    vector = pltpu.VMEM((1, WIDTH), F32)
    scratch = [
        pltpu.VMEM((HEADS, 64), F32),
        pltpu.VMEM((HEADS, 64), F32),
        pltpu.VMEM((4, FINE, WIDTH // 2), F32),
        pltpu.VMEM((1, ROWS), jnp.int32),
        vector,
        vector,
        vector,
        vector,
        vector,
        vector,
        pltpu.VMEM((ROWS, WIDTH), BF16),
        weight,
        weight,
        weight,
        weight,
        pltpu.VMEM((N_MP, HALF, WIDTH), BF16),
        pltpu.VMEM((WIDTH, WIDTH), BF16),
        pltpu.VMEM((WIDTH, WIDTH), BF16),
        pltpu.VMEM((WIDTH, words), BF16),
        pltpu.VMEM((HALF, WIDTH), BF16),
        pltpu.VMEM((WIDTH + BLOCK, HALF), BF16),
        pltpu.VMEM((ROWS, HALF), BF16),
        pltpu.VMEM((ROWS, HALF), BF16),
        kv,
        kv,
        kv,
        kv,
        kv,
        kv,
        pltpu.VMEM((HEADS, ROWS, ROWS), F32),
        pltpu.VMEM((HEADS, ROWS, ROWS), BF16),
        column,
        column,
        pltpu.VMEM((ROWS, HALF), F32),
        pltpu.VMEM((N_MP, ROWS, HALF), BF16),
        pltpu.VMEM((ROWS, WIDTH), BF16),
        pltpu.VMEM((BLOCK, WIDTH), BF16),
        pltpu.VMEM((4, N_MP, PIECE, WIDTH), BF16),
        pltpu.VMEM((4, N_MP - 1, PIECE, WIDTH), BF16),
        pltpu.VMEM((4, N_MP, PIECE, WIDTH), BF16),
        pltpu.VMEM((ROWS, 8), F32),
        pltpu.VMEM((N_MP, 8, ROWS), F32),
        pltpu.VMEM((2 * N_X, 8, BLOCK), F32),
        pltpu.VMEM((n_z, 8, BLOCK), F32),
        dma((19,)),
    ]
    scratch += [dma((4,))] * 8
    scratch += [dma((N_MP - 1,))] * 4
    scratch += [dma((N_MP - 1, 4))] * 6
    scratch += [dma((N_MP - 1,))] * 2
    scratch += [dma((2 * N_X - 1,))] * 2
    scratch += [dma((n_z - 1,))] * 2
    token_terms, docs = pl.pallas_call(
        functools.partial(kernel, n_seg),
        out_shape=(
            pltpu.VMEM((1, ROWS), F32),
            pltpu.VMEM((1, BLOCK), F32),
        ),
        in_specs=[vmem] * 3 + [hbm] * 19,
        out_specs=(vmem, vmem),
        scratch_shapes=scratch,
        compiler_params=pltpu.CompilerParams(
            collective_id=0, has_side_effects=True, vmem_limit_bytes=60 * 1024 * 1024
        ),
        name="layer",
    )(
        pred_device.reshape(1, 1),
        doc_ids.reshape(1, 1),
        valid_rows.reshape(1, 1),
        content_bias,
        position_bias,
        jnp.asarray(angle_basis()),
        targets.reshape(1, ROWS),
        attn_gain.reshape(1, WIDTH),
        attn_shift.reshape(1, WIDTH),
        up_bias.reshape(1, WIDTH),
        down_bias.reshape(1, WIDTH),
        ffn_gain.reshape(1, WIDTH),
        ffn_shift.reshape(1, WIDTH),
        embedded,
        w_query,
        w_key,
        w_value,
        w_rel,
        attn_out,
        w_up,
        w_down,
        w_vocab,
    )
    doc_slots = n_seg // 4
    token_terms, docs = pl.pallas_call(
        hand_over,
        out_shape=(
            jax.ShapeDtypeStruct((1, ROWS), F32),
            jax.ShapeDtypeStruct((1, doc_slots), F32),
        ),
        in_specs=[vmem, vmem],
        out_specs=(vmem, vmem),
        name="results",
    )(
        pltpu.with_memory_space_constraint(token_terms, pltpu.VMEM),
        pltpu.with_memory_space_constraint(docs, pltpu.VMEM),
    )
    return token_terms.reshape(ROWS), docs.reshape(doc_slots)


def solution(mesh):
    return jax.shard_map(
        functools.partial(on_device, mesh.shape["seg"]),
        mesh=mesh,
        in_specs=(
            P("seg", None),
            P("seg"),
            P("seg"),
            P("seg"),
            P("seg"),
            P(None, "mp"),
            P(None, "mp"),
            P(None, "mp"),
            P(None, "mp"),
            P("mp", None),
            P("mp", None),
            P("mp", None),
            P(),
            P(),
            P(None, "mp"),
            P("mp"),
            P("mp", None),
            P(),
            P(),
            P(),
            P(None, "mp"),
        ),
        out_specs=(P("seg"), P()),
        check_vma=False,
    )
```

```python
import functools

import jax
import jax.numpy as jnp
import numpy as np
from jax import lax
from jax.experimental import pallas as pl
from jax.experimental.pallas import tpu as pltpu
from jax.sharding import PartitionSpec as P

EPSILON = 1e-05
MESH = pl.DeviceIdType.MESH
F32, BF16 = jnp.float32, jnp.bfloat16
N_X = 4
N_MP = 4
HEADS = 4
ROWS = 512
WIDTH = 1024
BLOCK = 128
HALF = 256
PIECE = 32
FINE = 32
MASKED = -1e30


def normalize(values, gain, shift):
    centre = values - jnp.mean(values, axis=-1, keepdims=True)
    spread = jnp.mean(centre * centre, axis=-1, keepdims=True)
    return centre * lax.rsqrt(spread + EPSILON) * gain + shift


def dot(a, b):
    return jnp.dot(a, b, preferred_element_type=F32)


def dot_t(a, b):
    return lax.dot_general(a, b, (((1,), (1,)), ((), ())), preferred_element_type=F32)


def kernel(
    n_seg,
    pred_v,
    doc_v,
    valid_v,
    content_bias_h,
    position_bias_h,
    basis_h,
    targets_h,
    attn_gain_h,
    attn_shift_h,
    up_bias_h,
    down_bias_h,
    ffn_gain_h,
    ffn_shift_h,
    embedded_h,
    wq_h,
    wk_h,
    wv_h,
    wr_h,
    attn_out_h,
    wup_h,
    wdown_h,
    wvocab_h,
    token_o,
    doc_o,
    content_bias,
    position_bias,
    basis,
    targets,
    attn_gain,
    attn_shift,
    up_bias,
    down_bias,
    ffn_gain,
    ffn_shift,
    emb,
    wq,
    wk,
    wv,
    wr,
    attn_out,
    wup,
    wdown,
    wvocab,
    table,
    rel,
    qc,
    qp,
    kv_own,
    kv_same,
    kv_partner,
    kv_cross,
    kv_x,
    kv_past,
    pos_past,
    weights,
    top_own,
    sum_own,
    out_own,
    attended,
    first_out,
    units,
    rs_send,
    rs_recv,
    second,
    target_col,
    stats,
    doc_a,
    doc_b,
    load_sem,
    same_s,
    same_r,
    partner_s,
    partner_r,
    cross_s,
    cross_r,
    x_s,
    x_r,
    ao_s,
    ao_r,
    aof_s,
    aof_r,
    att_s,
    att_r,
    rs_s,
    rs_r,
    ag_s,
    ag_r,
    st_s,
    st_r,
    da_s,
    da_r,
    db_s,
    db_r,
):
    seg = lax.axis_index("seg")
    mp = lax.axis_index("mp")
    core = lax.rem(seg, 2)
    chip = lax.div(seg, 2)
    n_chip = n_seg // 2
    group = 2 * N_X
    n_z = n_seg // group
    in_group = lax.rem(seg, group)
    z = lax.div(seg, group)

    def chip_at(step, c):
        return (lax.rem(chip + step + n_chip, n_chip) * 2 + c, mp)

    partner = (chip * 2 + 1 - core, mp)
    forward = chip_at(1, core)
    backward = chip_at(-1, core)

    def mp_at(k):
        return (seg, lax.rem(mp + k, N_MP))

    def group_at(k):
        return (z * group + lax.rem(in_group + k, group), mp)

    def z_at(k):
        return (lax.rem(z + k, n_z) * group + in_group, mp)

    x_to = (lax.rem(chip + n_chip + 2 * core - 1, n_chip) * 2 + 1 - core, mp)

    pending = []

    def remote(src, dst, s_sem, r_sem, device):
        return pltpu.make_async_remote_copy(
            src_ref=src,
            dst_ref=dst,
            send_sem=s_sem,
            recv_sem=r_sem,
            device_id=device,
            device_id_type=MESH,
        )

    def send(*args):
        copy = remote(*args)
        copy.start()
        pending.append(copy)

    sources = (
        (embedded_h, emb),
        (wk_h, wk),
        (wv_h, wv),
        (attn_out_h, attn_out.at[mp]),
        (wq_h, wq),
        (wr_h, wr),
        (wup_h, wup),
        (wdown_h, wdown),
        (wvocab_h, wvocab),
        (content_bias_h, content_bias),
        (position_bias_h, position_bias),
        (basis_h, basis),
        (targets_h, targets),
        (attn_gain_h, attn_gain),
        (attn_shift_h, attn_shift),
        (up_bias_h, up_bias),
        (down_bias_h, down_bias),
        (ffn_gain_h, ffn_gain),
        (ffn_shift_h, ffn_shift),
    )
    loads = [pltpu.make_async_copy(src, dst, load_sem.at[n]) for n, (src, dst) in enumerate(sources)]
    for n in (0, 1, 2, 4, 9, 10, 11, 5, 3, *range(12, 19)):
        loads[n].start()

    barrier = pltpu.get_barrier_semaphore()
    friends = [partner, forward, backward, x_to]
    friends += [mp_at(k) for k in range(1, N_MP)]
    friends += [group_at(k) for k in range(1, group)]
    friends += [z_at(k) for k in range(1, n_z)]
    for friend in friends:
        pl.semaphore_signal(barrier, inc=1, device_id=friend, device_id_type=MESH)

    def kv_sends(t):
        send(kv_own.at[t], kv_same.at[t], same_s.at[t], same_r.at[t], forward)
        send(kv_own.at[t], kv_partner.at[t], partner_s.at[t], partner_r.at[t], partner)

        @pl.when(core == 0)
        def _():
            remote(kv_own.at[t], kv_x.at[t], x_s.at[t], x_r.at[t], x_to).start()

    loads[0].wait()
    loads[1].wait()
    for t in range(2):
        kv_own[t] = dot(emb[t * HALF : (t + 1) * HALF, :], wk[...]).astype(BF16)
    pl.semaphore_wait(barrier, len(friends))
    for t in range(2):
        kv_sends(t)
    loads[2].wait()
    for t in range(2):
        kv_own[2 + t] = dot(emb[t * HALF : (t + 1) * HALF, :], wv[...]).astype(BF16)
    for t in range(2, 4):
        kv_sends(t)

    loads[3].wait()
    for n in (6, 7, 8):
        loads[n].start()
    part = pl.ds(pl.multiple_of(core * BLOCK, BLOCK), BLOCK)
    for k in range(1, N_MP):
        here = attn_out.at[mp, part]
        send(here, here, ao_s.at[k - 1], ao_r.at[k - 1], mp_at(k))

    loads[4].wait()
    loads[9].wait()
    loads[10].wait()
    for t in range(2):
        rows = slice(t * HALF, (t + 1) * HALF)
        q = dot(emb[rows, :], wq[...])
        for h in range(HEADS):
            cols = slice(h * 64, (h + 1) * 64)
            qc[rows, cols] = (q[:, cols] + content_bias[h : h + 1, :]).astype(BF16)
            qp[rows, cols] = (q[:, cols] + position_bias[h : h + 1, :]).astype(BF16)

    loads[5].wait()
    loads[11].wait()
    rel[WIDTH:, :] = jnp.zeros((BLOCK, HALF), BF16)

    def rel_block(n, carry):
        for k in range(HALF // FINE):
            at = n * (HALF // FINE) + k
            sin_a, cos_a = basis[0, pl.ds(at, 1), :], basis[1, pl.ds(at, 1), :]
            sin_b, cos_b = basis[2], basis[3]
            rows = slice(k * FINE, (k + 1) * FINE)
            table[rows, : WIDTH // 2] = (sin_a * cos_b + cos_a * sin_b).astype(BF16)
            table[rows, WIDTH // 2 :] = (cos_a * cos_b - sin_a * sin_b).astype(BF16)
        rel[pl.ds(pl.multiple_of(n * HALF, HALF), HALF), :] = dot(table[...], wr[...]).astype(BF16)
        return carry

    lax.fori_loop(0, WIDTH // HALF, rel_block, 0)

    lanes = lax.broadcasted_iota(jnp.int32, (BLOCK, HALF), 1)
    row_at = lax.broadcasted_iota(jnp.int32, (BLOCK, BLOCK), 0)
    col_at = lax.broadcasted_iota(jnp.int32, (BLOCK, BLOCK), 1)

    def of_head(h):
        return (lanes >= h * 64) & (lanes < h * 64 + 64)

    def one_head(ref, rows, mine):
        values = ref[rows, :].astype(F32) * 0.125
        return jnp.where(mine, values, 0.0).astype(BF16)

    def relay(t):
        remote(kv_own.at[t], kv_same.at[t], same_s.at[t], same_r.at[t], forward).wait_recv()
        send(kv_same.at[t], kv_cross.at[t], cross_s.at[t], cross_r.at[t], partner)

        @pl.when(core == 1)
        def _():
            remote(kv_same.at[t], kv_x.at[t], x_s.at[t], x_r.at[t], x_to).start()

    for b in range(ROWS // BLOCK):
        rows = slice(b * BLOCK, (b + 1) * BLOCK)
        own = (b + 1) * BLOCK
        begin = ROWS - own
        width = WIDTH + BLOCK - begin

        keys = []
        for c in range(2):
            if own > c * HALF:
                keys.append((c, min(HALF, own - c * HALF)))
        outcome = None
        for h in range(HEADS):
            mine = of_head(h)
            near = dot_t(one_head(qp, rows, mine), rel[begin:, :])
            near = pltpu.roll(near, width - BLOCK + 1, 1, stride=1, stride_axis=0)
            pos_past[h, rows, :] = near[:, :ROWS]
            query = one_head(qc, rows, mine)
            content = [dot_t(query, kv_own[c, :n, :]) for c, n in keys]
            content = content[0] if len(content) == 1 else jnp.concatenate(content, axis=1)
            score = content + near[:, ROWS : ROWS + own]
            last = jnp.where(col_at <= row_at, score[:, own - BLOCK :], MASKED)
            score = last if own == BLOCK else jnp.concatenate([score[:, : own - BLOCK], last], axis=1)
            top = jnp.max(score, axis=-1, keepdims=True)
            weight = jnp.exp(score - top)
            top_own[h, rows, :] = top
            sum_own[h, rows, :] = jnp.sum(weight, axis=-1, keepdims=True)
            weight = weight.astype(BF16)
            total = None
            for c, n in keys:
                term = dot(weight[:, c * HALF : c * HALF + n], kv_own[2 + c, :n, :])
                total = term if total is None else total + term
            outcome = total if outcome is None else jnp.where(mine, total, outcome)
        out_own[rows, :] = outcome
        relay(b)

    for k in range(1, N_MP):
        there = lax.rem(mp + N_MP - k, N_MP)
        here = attn_out.at[there, part]
        remote(here, here, ao_s.at[k - 1], ao_r.at[k - 1], mp_at(k)).wait_recv()
        send(here, here, aof_s.at[k - 1], aof_r.at[k - 1], partner)

    for n in range(12, 19):
        loads[n].wait()
    spread = jnp.broadcast_to(targets[...].astype(F32), (BLOCK, ROWS))
    target_col[...] = jnp.transpose(spread)[:, :8]
    previous = pred_v[...]
    behind = jnp.broadcast_to(seg - previous, (HALF, HALF))
    has_memory = jnp.broadcast_to(previous, (BLOCK, ROWS)) >= 0
    use_cross = behind == 1 + 2 * core
    use_partner = behind == 2 * core - 1
    use_x = behind == 3 - 4 * core

    def choose(t):
        remote(kv_own.at[t], kv_partner.at[t], partner_s.at[t], partner_r.at[t], partner).wait_recv()
        remote(kv_same.at[t], kv_cross.at[t], cross_s.at[t], cross_r.at[t], partner).wait_recv()
        remote(kv_same.at[t], kv_x.at[t], x_s.at[t], x_r.at[t], x_to).wait_recv()
        chosen = jnp.where(use_cross, kv_cross[t], kv_same[t])
        chosen = jnp.where(use_partner, kv_partner[t], chosen)
        kv_past[t] = jnp.where(use_x, kv_x[t], chosen)

    def origin(k):
        return lax.rem(mp + N_MP - k, N_MP)

    def attended_copy(b, k, owner):
        here = attended.at[owner, b * BLOCK : (b + 1) * BLOCK]
        return remote(here, here, att_s.at[k - 1, b], att_r.at[k - 1, b], mp_at(k))

    def reduce_copy(b, k):
        src = rs_send.at[b, lax.rem(mp + k, N_MP)]
        return remote(src, rs_recv.at[b, k - 1], rs_s.at[k - 1, b], rs_r.at[k - 1, b], mp_at(k))

    def second_copy(b, k, owner):
        here = second.at[b, owner]
        return remote(here, here, ag_s.at[k - 1, b], ag_r.at[k - 1, b], mp_at(k))

    def begin(copy):
        copy.start()
        pending.append(copy)

    def weigh(b):
        rows = slice(b * BLOCK, (b + 1) * BLOCK)
        for h in range(HEADS):
            query = one_head(qc, rows, of_head(h))
            score = jnp.concatenate([dot_t(query, kv_past[c]) for c in range(2)], axis=1)
            score = jnp.where(has_memory, score + pos_past[h, rows, :], MASKED)
            before = top_own[h, rows, :]
            top = jnp.maximum(before, jnp.max(score, axis=-1, keepdims=True))
            weight = jnp.exp(score - top)
            fade = jnp.exp(before - top)
            sum_own[h, rows, :] = sum_own[h, rows, :] * fade + jnp.sum(weight, axis=-1, keepdims=True)
            top_own[h, rows, :] = fade
            weights[h, rows, :] = weight.astype(BF16)

    def attend(b):
        rows = slice(b * BLOCK, (b + 1) * BLOCK)
        outcome = None
        for h in range(HEADS):
            past = dot(weights[h, rows, :HALF], kv_past[2]) + dot(weights[h, rows, HALF:], kv_past[3])
            done = (out_own[rows, :] * top_own[h, rows, :] + past) / sum_own[h, rows, :]
            outcome = done if outcome is None else jnp.where(of_head(h), done, outcome)
        attended[mp, rows, :] = outcome.astype(BF16)
        for k in (2, 1, 3):
            begin(attended_copy(b, k, mp))

    def feed(b):
        rows = slice(b * BLOCK, (b + 1) * BLOCK)
        for k in range(1, N_MP):
            attended_copy(b, k, origin(k)).wait_recv()
        head_sum = None
        for g in range(N_MP):
            term = dot(attended[g, rows, :], attn_out[g]).astype(BF16).astype(F32)
            head_sum = term if head_sum is None else head_sum + term
        total = emb[rows, :].astype(F32) + head_sum
        first = normalize(total, attn_gain[...], attn_shift[...]).astype(BF16)
        first_out[rows, :] = first
        units[...] = jnp.maximum(dot(first, wup[...]) + up_bias[...], 0.0).astype(BF16)
        terms = dot(units[...], wdown[...]).astype(BF16)
        for d in range(N_MP):
            rs_send[b, d] = terms[d * PIECE : (d + 1) * PIECE, :]
        for k in (2, 1, 3):
            begin(reduce_copy(b, k))

    def finish_reduce(b):
        total = rs_send[b, mp].astype(F32)
        for k in range(1, N_MP):
            reduce_copy(b, k).wait_recv()
            total = total + rs_recv[b, k - 1].astype(F32)
        at = pl.ds(pl.multiple_of(b * BLOCK + mp * PIECE, PIECE), PIECE)
        total = first_out[at, :].astype(F32) + total + down_bias[...]
        second[b, mp] = normalize(total, ffn_gain[...], ffn_shift[...]).astype(BF16)
        for k in (2, 1, 3):
            begin(second_copy(b, k, mp))

    def second_arrived(b):
        for k in range(1, N_MP):
            second_copy(b, k, origin(k)).wait_recv()

    choose(0)
    choose(1)
    weigh(0)
    weigh(1)
    choose(2)
    choose(3)
    attend(0)
    attend(1)
    weigh(2)
    attend(2)
    for k in range(1, N_MP):
        there = lax.rem(mp + N_MP - k, N_MP)
        other = pl.ds(pl.multiple_of((1 - core) * BLOCK, BLOCK), BLOCK)
        here = attn_out.at[there, other]
        remote(here, here, aof_s.at[k - 1], aof_r.at[k - 1], partner).wait_recv()
    for n in (6, 7, 8):
        loads[n].wait()
    weigh(3)
    attend(3)
    feed(0)
    feed(1)
    feed(2)
    finish_reduce(0)
    feed(3)
    finish_reduce(1)
    finish_reduce(2)

    tile = 512
    n_words = wvocab_h.shape[1]
    for blocks in ((0, 1), (2,), (3,)):
        count = len(blocks) * BLOCK
        rows = slice(blocks[0] * BLOCK, blocks[0] * BLOCK + count)
        for b in blocks:
            second_arrived(b)
        states = [second[b, d] for b in blocks for d in range(N_MP)]
        states = jnp.concatenate(states, axis=0)
        wanted = target_col[rows, 0:1].astype(jnp.int32) - mp * n_words
        words = lax.broadcasted_iota(jnp.int32, (count, tile), 1)

        def vocab_tile(n, carry, states=states, wanted=wanted, words=words):
            top, total, picked = carry
            at = pl.multiple_of(n * tile, tile)
            logits = dot(states, wvocab[:, pl.ds(at, tile)])
            new_top = jnp.maximum(top, jnp.max(logits, axis=1, keepdims=True))
            total = total * jnp.exp(top - new_top)
            total = total + jnp.sum(jnp.exp(logits - new_top), axis=1, keepdims=True)
            hit = jnp.where(words == wanted - at, logits, 0.0)
            return new_top, total, picked + jnp.sum(hit, axis=1, keepdims=True)

        zero = jnp.zeros((count, 1), F32)
        found = (jnp.full((count, 1), -jnp.inf, F32), zero, zero)
        found = lax.fori_loop(0, 2, vocab_tile, found)
        if blocks[0] == 0:
            finish_reduce(3)
        top, total, picked = lax.fori_loop(2, n_words // tile, vocab_tile, found)
        lane = lax.broadcasted_iota(jnp.int32, (count, BLOCK), 1)
        packed = jnp.where(lane == 0, top, jnp.where(lane == 1, total, picked))
        stats[mp, :, rows] = jnp.transpose(packed)[:8, :]

    for k in range(1, N_MP):
        here = stats.at[mp]
        send(here, here, st_s.at[k - 1], st_r.at[k - 1], mp_at(k))
    for k in range(1, N_MP):
        there = lax.rem(mp + N_MP - k, N_MP)
        here = stats.at[there]
        remote(here, here, st_s.at[k - 1], st_r.at[k - 1], mp_at(k)).wait_recv()
    top = stats[0, 0:1, :]
    for g in range(1, N_MP):
        top = jnp.maximum(top, stats[g, 0:1, :])
    total, picked = None, None
    for g in range(N_MP):
        term = stats[g, 1:2, :] * jnp.exp(stats[g, 0:1, :] - top)
        total = term if total is None else total + term
        picked = stats[g, 2:3, :] if picked is None else picked + stats[g, 2:3, :]
    position = lax.broadcasted_iota(jnp.int32, (1, ROWS), 1)
    tokens = jnp.where(position < jnp.broadcast_to(valid_v[...], (1, ROWS)), picked - (top + jnp.log(total)), 0.0)
    token_o[...] = tokens

    slot = lax.broadcasted_iota(jnp.int32, (8, BLOCK), 1) == jnp.broadcast_to(doc_v[...], (8, BLOCK))
    line = lax.broadcasted_iota(jnp.int32, (8, BLOCK), 0)
    used = valid_v[...].astype(F32)
    share = jnp.sum(tokens, axis=1, keepdims=True)
    doc_a[0] = jnp.where(slot, jnp.where(line == 0, share, jnp.where(line == 1, used, 0.0)), 0.0)
    for k in range(1, group):
        send(doc_a.at[0], doc_a.at[k], da_s.at[k - 1], da_r.at[k - 1], group_at(k))
    for k in range(1, group):
        remote(doc_a.at[0], doc_a.at[k], da_s.at[k - 1], da_r.at[k - 1], group_at(k)).wait_recv()
    doc_b[0] = jnp.sum(doc_a[...], axis=0)
    earlier = list(pending)
    for k in range(1, n_z):
        send(doc_b.at[0], doc_b.at[k], db_s.at[k - 1], db_r.at[k - 1], z_at(k))
    for copy in earlier:
        copy.wait_send()
    for t in range(4):
        remote(kv_own.at[t], kv_x.at[t], x_s.at[t], x_r.at[t], x_to).wait_send()
    for k in range(1, n_z):
        remote(doc_b.at[0], doc_b.at[k], db_s.at[k - 1], db_r.at[k - 1], z_at(k)).wait_recv()
    docs = jnp.sum(doc_b[...], axis=0)
    doc_o[...] = docs[0:1, :] / docs[1:2, :]
    for copy in pending[len(earlier) :]:
        copy.wait_send()


def hand_over(token_i, doc_i, token_o, doc_o):
    token_o[...] = token_i[...]
    doc_o[...] = doc_i[:, : doc_o.shape[1]]


def angle_basis():
    frequency = 10000.0 ** (-np.arange(0, WIDTH, 2, dtype=np.float64) / WIDTH)
    coarse = (WIDTH // FINE - 1 - np.arange(WIDTH // FINE))[:, None] * FINE * frequency[None, :]
    fine = (FINE - 1 - np.arange(FINE))[:, None] * frequency[None, :]
    return np.stack([np.sin(coarse), np.cos(coarse), np.sin(fine), np.cos(fine)]).astype(np.float32)


def on_device(
    n_seg,
    embedded,
    targets,
    pred_device,
    doc_ids,
    valid_rows,
    w_query,
    w_key,
    w_value,
    w_rel,
    content_bias,
    position_bias,
    attn_out,
    attn_gain,
    attn_shift,
    w_up,
    up_bias,
    w_down,
    down_bias,
    ffn_gain,
    ffn_shift,
    w_vocab,
):
    vmem = pl.BlockSpec(memory_space=pltpu.VMEM)
    hbm = pl.BlockSpec(memory_space=pltpu.HBM)
    dma = pltpu.SemaphoreType.DMA
    words = w_vocab.shape[1]
    n_z = n_seg // (2 * N_X)
    kv = pltpu.VMEM((4, HALF, HALF), BF16)
    weight = pltpu.VMEM((WIDTH, HALF), BF16)
    column = pltpu.VMEM((HEADS, ROWS, 1), F32)
    vector = pltpu.VMEM((1, WIDTH), F32)
    scratch = [
        pltpu.VMEM((HEADS, 64), F32),
        pltpu.VMEM((HEADS, 64), F32),
        pltpu.VMEM((4, FINE, WIDTH // 2), F32),
        pltpu.VMEM((1, ROWS), jnp.int32),
        vector,
        vector,
        vector,
        vector,
        vector,
        vector,
        pltpu.VMEM((ROWS, WIDTH), BF16),
        weight,
        weight,
        weight,
        weight,
        pltpu.VMEM((N_MP, HALF, WIDTH), BF16),
        pltpu.VMEM((WIDTH, WIDTH), BF16),
        pltpu.VMEM((WIDTH, WIDTH), BF16),
        pltpu.VMEM((WIDTH, words), BF16),
        pltpu.VMEM((HALF, WIDTH), BF16),
        pltpu.VMEM((WIDTH + BLOCK, HALF), BF16),
        pltpu.VMEM((ROWS, HALF), BF16),
        pltpu.VMEM((ROWS, HALF), BF16),
        kv,
        kv,
        kv,
        kv,
        kv,
        kv,
        pltpu.VMEM((HEADS, ROWS, ROWS), F32),
        pltpu.VMEM((HEADS, ROWS, ROWS), BF16),
        column,
        column,
        pltpu.VMEM((ROWS, HALF), F32),
        pltpu.VMEM((N_MP, ROWS, HALF), BF16),
        pltpu.VMEM((ROWS, WIDTH), BF16),
        pltpu.VMEM((BLOCK, WIDTH), BF16),
        pltpu.VMEM((4, N_MP, PIECE, WIDTH), BF16),
        pltpu.VMEM((4, N_MP - 1, PIECE, WIDTH), BF16),
        pltpu.VMEM((4, N_MP, PIECE, WIDTH), BF16),
        pltpu.VMEM((ROWS, 8), F32),
        pltpu.VMEM((N_MP, 8, ROWS), F32),
        pltpu.VMEM((2 * N_X, 8, BLOCK), F32),
        pltpu.VMEM((n_z, 8, BLOCK), F32),
        dma((19,)),
    ]
    scratch += [dma((4,))] * 8
    scratch += [dma((N_MP - 1,))] * 4
    scratch += [dma((N_MP - 1, 4))] * 6
    scratch += [dma((N_MP - 1,))] * 2
    scratch += [dma((2 * N_X - 1,))] * 2
    scratch += [dma((n_z - 1,))] * 2
    token_terms, docs = pl.pallas_call(
        functools.partial(kernel, n_seg),
        out_shape=(
            pltpu.VMEM((1, ROWS), F32),
            pltpu.VMEM((1, BLOCK), F32),
        ),
        in_specs=[vmem] * 3 + [hbm] * 19,
        out_specs=(vmem, vmem),
        scratch_shapes=scratch,
        compiler_params=pltpu.CompilerParams(
            collective_id=0, has_side_effects=True, vmem_limit_bytes=60 * 1024 * 1024
        ),
        name="layer",
    )(
        pred_device.reshape(1, 1),
        doc_ids.reshape(1, 1),
        valid_rows.reshape(1, 1),
        content_bias,
        position_bias,
        jnp.asarray(angle_basis()),
        targets.reshape(1, ROWS),
        attn_gain.reshape(1, WIDTH),
        attn_shift.reshape(1, WIDTH),
        up_bias.reshape(1, WIDTH),
        down_bias.reshape(1, WIDTH),
        ffn_gain.reshape(1, WIDTH),
        ffn_shift.reshape(1, WIDTH),
        embedded,
        w_query,
        w_key,
        w_value,
        w_rel,
        attn_out,
        w_up,
        w_down,
        w_vocab,
    )
    doc_slots = n_seg // 4
    token_terms, docs = pl.pallas_call(
        hand_over,
        out_shape=(
            jax.ShapeDtypeStruct((1, ROWS), F32),
            jax.ShapeDtypeStruct((1, doc_slots), F32),
        ),
        in_specs=[vmem, vmem],
        out_specs=(vmem, vmem),
        name="results",
    )(
        pltpu.with_memory_space_constraint(token_terms, pltpu.VMEM),
        pltpu.with_memory_space_constraint(docs, pltpu.VMEM),
    )
    return token_terms.reshape(ROWS), docs.reshape(doc_slots)


def solution(mesh):
    return jax.shard_map(
        functools.partial(on_device, mesh.shape["seg"]),
        mesh=mesh,
        in_specs=(
            P("seg", None),
            P("seg"),
            P("seg"),
            P("seg"),
            P("seg"),
            P(None, "mp"),
            P(None, "mp"),
            P(None, "mp"),
            P(None, "mp"),
            P("mp", None),
            P("mp", None),
            P("mp", None),
            P(),
            P(),
            P(None, "mp"),
            P("mp"),
            P("mp", None),
            P(),
            P(),
            P(),
            P(None, "mp"),
        ),
        out_specs=(P("seg"), P()),
        check_vma=False,
    )
```
